32 devices in a mesh: groups: 2 (over x), elem: 16 (over z, y, core).
Axes of the slice: x: 2, y: 2, z: 4, core: 2. Of those that a mesh axis runs over, the one named last changes fastest.
Arguments:
- snapshots: float32 [2, 4096, 16384], P(None, ('groups', 'elem')), parts along dimension 1, may hold values from -6 to 6
- delays: float32 [384, 2048], replicated, may hold values from -3 to 3
- element_order: int32 [4096], P('groups'), parts along dimension 0, may hold values from 0 to 2047, each once
- beam_table: int32 [512], P('groups'), parts along dimension 0, may hold values from 0 to 383
- band_len: int32 [8], replicated, may hold values from 1 to 4, 16 in all
Outputs:
- beams: float32 [16384, 2, 512], P('elem', None, 'groups'), parts along dimension 2
- power_db: float32 [8, 512], P(None, 'groups'), parts along dimension 1
The draws below stay inside these ranges and needn't reach their ends.
There are 2 independent parts, one for each index of `groups`. The reference program is written for one: setup_inputs(seed, part) draws one part's arguments, and reference() takes and returns one part's arrays. A program takes and returns all parts, laid end to end along the dimension named above; an argument that names none is the same for every part. Nothing has to cross between parts.
Inputs may be any that keep to these rules, and one draw needn't show every extreme that they name: `element_order`: each of 0 to 2047 appears once. `band_len`: the entries sum to 16.
All inputs are finite; a program needn't handle non-finite values.
Results may differ from the reference program's by a relative error of at most 0.0003.
Values sent between devices are 32-bit elements; how exact they have to be, the bound alone decides.
A program may use at most 128 MiB of HBM per device.

```python
import math
import jax
import jax.numpy as jnp
import numpy as np
from jax import lax

E = 2048
BEAMS = 256
DIRS = 384
BANDS = 8
UNITS = 16
BAND_MOST = 4
COLS = 16384


def place_ends(drawn, key, least, high):
    longest = drawn.shape.index(max(drawn.shape))
    spots = []
    for shift in (0, 1):
        where = [jax.random.randint(jax.random.fold_in(key, axis), (), 0, length) for axis, length in enumerate(drawn.shape)]
        where[longest] = (where[longest] + shift) % drawn.shape[longest]
        spots.append(tuple(where))
    return drawn.at[spots[0]].set(least).at[spots[1]].set(high)


def levels(key, dims, pieces, least, largest):
    factor_of, own = 1.0, jax.random.fold_in(key, 6)
    for dim, shards_of in pieces:
        draws = jnp.exp(jax.random.uniform(jax.random.fold_in(own, dim), (shards_of,), jnp.float32, least / len(pieces), largest / len(pieces)))
        factor_of = factor_of * jnp.repeat(draws, dims[dim] // shards_of).reshape([-1 if axis == dim else 1 for axis in range(len(dims))])
    return factor_of


def profile(number_of, total, limit, lean):
    loads = [(1 << 20) // math.isqrt(rank ** lean) + 1 for rank in range(2, number_of + 1)]
    rest, holding = total - limit - (number_of - 1), [1] * (number_of - 1)
    while rest > 0:
        movable = [i for i in range(number_of - 1) if holding[i] < limit]
        whole, budget = sum([loads[i] for i in movable]), rest
        for i in movable:
            more = min(limit - holding[i], max(1, budget * loads[i] // whole), rest)
            holding[i] = holding[i] + more
            rest = rest - more
    return np.array([limit] + holding)


def uneven_parts(stream_key, amount, total, most, lean):
    if amount == 2:
        one = jax.random.randint(stream_key, (), max(1, total - most), min(most, total - 1) + 1)
        return jnp.stack([one, total - one])
    sizes = jnp.asarray(profile(amount, total, most, lean), jnp.int32)
    couples = (amount - 1) // 2
    giver, taker = sizes[1:1 + 2 * couples:2], sizes[2:2 + 2 * couples:2]
    slack = jnp.minimum(giver - 1, most - taker)
    passed = jax.random.randint(jax.random.fold_in(stream_key, 1), (couples,), 0, 1 << 20) % (slack + 1)
    sizes = sizes.at[1:1 + 2 * couples:2].set(giver - passed).at[2:2 + 2 * couples:2].set(taker + passed)
    return sizes[jax.random.permutation(jax.random.fold_in(stream_key, 2), amount)]


def bell_draw(stream_key, dims, scale, most, split=(), held_as=jnp.bfloat16):
    gain = levels(stream_key, dims, split, -0.22, 0.18) if split else 1.0
    entries = jax.random.normal(stream_key, dims, jnp.float32) * scale * gain
    return jnp.minimum(jnp.maximum(entries, -most), most).astype(held_as)


def setup_inputs(seed: int = 0, part: int = 0) -> dict:
    splits = jax.random.split(jax.random.key(seed), 6)
    own_keys = jax.random.split(jax.random.fold_in(splits[5], part), 6)
    return {
        "snapshots": bell_draw(own_keys[0], (2, E, COLS), 1.0, 6.0, ((1, 16),), jnp.float32),
        "delays": jnp.clip(jax.random.uniform(splits[1], (DIRS, E), jnp.float32, -3.0, 3.0), -3.0, 3.0),
        "element_order": jax.random.permutation(own_keys[2], E).astype(jnp.int32),
        "beam_table": place_ends(jax.random.randint(own_keys[3], (BEAMS,), 0, DIRS), jax.random.fold_in(own_keys[3], 1), 0, DIRS - 1).astype(jnp.int32),
        "band_len": uneven_parts(splits[4], BANDS, UNITS, BAND_MOST, 2).astype(jnp.int32),
    }


epsilon = 1e-6


def band_of(band_len, position, unit_count):
    band_ends = jnp.cumsum(band_len).astype(jnp.int32)
    band_index = jnp.sum((band_ends <= position).astype(jnp.int32)).astype(jnp.int32)
    selector = jnp.arange(band_len.shape[0], dtype=jnp.int32) == band_index
    band_size = jnp.sum(jnp.where(selector, band_len, 0)).astype(jnp.int32)
    band_start = (jnp.sum(jnp.where(selector, band_ends, 0)).astype(jnp.int32) - band_size).astype(jnp.int32)
    frequency = (band_start.astype(jnp.float32) + 0.5 * band_size.astype(jnp.float32)) / float(unit_count)
    return frequency, band_size, selector.astype(jnp.float32)


def steering(delays, element_order, beam_table, frequency):
    delay_rows = jnp.take(delays, beam_table, axis=0)
    delay_rows = jnp.take(delay_rows, element_order, axis=1)
    phases = (2.0 * math.pi * frequency) * delay_rows
    scaling = float(delays.shape[1]) ** -0.5
    cosines = jnp.cos(phases) * scaling
    sines = -jnp.sin(phases) * scaling
    upper_rows = jnp.concatenate([cosines.T, sines.T], axis=1)
    lower_rows = jnp.concatenate([-sines.T, cosines.T], axis=1)
    return jnp.concatenate([upper_rows, lower_rows], axis=0)


def reference(snapshots, delays, element_order, beam_table, band_len):
    unit_cols = snapshots.shape[2] // UNITS
    stacked_rows = 2 * snapshots.shape[1]
    beam_count = beam_table.shape[0]

    def one_unit(position):
        frequency, band_size, selector = band_of(band_len, position, UNITS)
        weights = steering(delays, element_order, beam_table, frequency)
        window = lax.dynamic_slice_in_dim(snapshots, position * unit_cols, unit_cols, 2)
        formed = lax.dot_general(window.reshape(stacked_rows, unit_cols), weights, (((0,), (0,)), ((), ())), precision=lax.Precision.HIGHEST, preferred_element_type=jnp.float32)
        squares = jnp.sum(formed * formed, axis=0)
        power_mean = (squares[:beam_count] + squares[beam_count:]) / (band_size.astype(jnp.float32) * unit_cols)
        return formed, selector[:, None] * power_mean[None, :]

    formed_all, partials = lax.map(one_unit, jnp.arange(UNITS, dtype=jnp.int32))
    beams = formed_all.reshape(snapshots.shape[2], 2, beam_count)
    mean_power = jnp.sum(partials, axis=0)
    return beams, 10.0 * jnp.log10(mean_power + epsilon)
```

```python
import functools
import math

import jax
import jax.numpy as jnp
from jax import lax
from jax.experimental import pallas as pl
from jax.experimental.pallas import tpu as pltpu
from jax.sharding import PartitionSpec as P

epsilon = 1e-06
SIDE = 2
RING = 4
CHUNKS = 8


def band_of(band_len, position, unit_count):
    band_ends = jnp.cumsum(band_len)
    band_index = jnp.sum((band_ends <= position).astype(jnp.int32))
    selector = jnp.arange(band_len.shape[0], dtype=jnp.int32) == band_index
    band_size = jnp.sum(jnp.where(selector, band_len, 0))
    band_start = jnp.sum(jnp.where(selector, band_ends, 0)) - band_size
    frequency = (band_start.astype(jnp.float32) + 0.5 * band_size.astype(jnp.float32)) / float(
        unit_count
    )
    return (frequency, band_size, selector.astype(jnp.float32))


def sincos(turns):
    reduced = turns - jnp.floor(turns + 0.5)
    x = reduced * math.pi
    q = x * x
    sin_terms = [(-1.0) ** i / math.factorial(2 * i + 1) for i in range(7)]
    cos_terms = [(-1.0) ** i / math.factorial(2 * i) for i in range(8)]
    s = jnp.full_like(q, sin_terms[-1])
    for term in sin_terms[-2::-1]:
        s = s * q + term
    s = s * x
    c = jnp.full_like(q, cos_terms[-1])
    for term in cos_terms[-2::-1]:
        c = c * q + term
    return 2.0 * s * c, 1.0 - 2.0 * s * s


def split2(v):
    high = v.astype(jnp.bfloat16)
    return high, (v - high.astype(jnp.float32)).astype(jnp.bfloat16)


def split3(v):
    high = v.astype(jnp.bfloat16)
    rest = v - high.astype(jnp.float32)
    middle = rest.astype(jnp.bfloat16)
    return high, middle, (rest - middle.astype(jnp.float32)).astype(jnp.bfloat16)


def item_unit(i):
    return 3 - i + (i + RING) // (RING + 1) + i // (RING + 1)


def item_chunk(i):
    return CHUNKS - 2 + (i + RING) // (RING + 1) - i // (RING + 1)


def kernel(
    n, lens, x, delays, order, table, out, power,
    bl, dl, od, tb, g1, dt, wh, wl, xa, xb, xz, pa, pb, ra, rb, ry, pw, tot,
    in_s, own_a, own_b, sa_s, sa_r, sb_s, sb_r, sy_s, sy_r, sz_s, sz_r,
    a_s, a_r, b_s, b_r, y2_s, y2_r, p_s, p_r,
):
    me = lax.axis_index("elem")
    core = me % SIDE
    y = (me // SIDE) % SIDE
    z = me // (SIDE * SIDE)
    upper = z // 2
    end = z + upper * (RING - 1 - 2 * z)
    unit_cols = x.shape[2] // n
    chunk = unit_cols // CHUNKS
    most = CHUNKS - 1
    beams = table.shape[1]
    scaling = float(delays.shape[1]) ** (-0.5)
    slots = (3, 2, 1 - end, end)
    early = (most - 1, most, most - end, most - 1 + end)

    def chip(u):
        return u + upper * (RING - 1 - 2 * u)

    def dev(zz, yy, cc):
        return (zz * SIDE + yy % SIDE) * SIDE + cc % SIDE

    ahead = dev(chip(end + 1), y, core)
    beside = dev(chip(1 - end), y, core)

    barrier = pltpu.get_barrier_semaphore()

    def greet(target):
        pl.semaphore_signal(barrier, inc=1, device_id={"elem": target},
                            device_id_type=pl.DeviceIdType.MESH)

    for r in (0, 1):
        greet(dev(z, y + 1, core + r))
        greet(dev(chip(1 - end), y, core + r))
    greet(dev(z, y, core + 1))

    @pl.when(end == 1)
    def _():
        greet(ahead)

    fetches = [
        pltpu.make_async_copy(lens, bl, in_s.at[0]),
        pltpu.make_async_copy(delays, dl, in_s.at[1]),
        pltpu.make_async_copy(order, od, in_s.at[2]),
        pltpu.make_async_copy(table, tb, in_s.at[3]),
    ]
    for fetch in fetches:
        fetch.start()
    pl.semaphore_wait(barrier, 5 + end)

    def remote(src, dst, send, recv, target):
        return pltpu.make_async_remote_copy(
            src_ref=src, dst_ref=dst, send_sem=send, recv_sem=recv,
            device_id={"elem": target}, device_id_type=pl.DeviceIdType.MESH)

    def cols(unit, start, size):
        return x.at[:, :, pl.ds(pl.multiple_of(unit * unit_cols + start, 128), size)]

    def part(k):
        return pl.ds(pl.multiple_of(k * chunk, 128), chunk)

    def y_copy(j, k, r):
        return remote(
            cols(dev(chip(slots[j]), y + 1, core + r), k * chunk, chunk),
            xa.at[2 + r, j, :, :, part(k)],
            sy_s.at[r, j, k], sy_r.at[r, j, k], dev(z, y + 1, core + r))

    def late(i, yy, cc):
        return cols(dev(chip(item_unit(i)), yy, cc), item_chunk(i) * chunk, chunk)

    def z_copy(i, yr, r):
        return remote(
            late(i, y + yr, core + r), xz.at[i, r, yr],
            sz_s.at[i, r, yr], sz_r.at[i, r, yr], dev(chip(1 - end), y, core + r))

    def b_peer(i, yr):
        return remote(late(i, y + yr, core + 1), xb.at[1, i, yr],
                      sb_s.at[i, yr], sb_r.at[i, yr], dev(z, y, core + 1))

    def b_own(i, yr):
        return pltpu.make_async_copy(late(i, y + yr, core), xb.at[0, i, yr], own_b.at[i, yr])

    def a_copy(j, k):
        to = j + 3 * end if j < 2 else 2
        return remote(pa.at[j, k], ra.at[to, k], a_s.at[j, k], a_r.at[to, k],
                      ahead if j < 2 else beside)

    def a_wait(to, k):
        remote(pa.at[0, k], ra.at[to, k], a_s.at[0, k], a_r.at[to, k], beside).wait_recv()

    def b_copy(i, yr):
        to = i if i < 3 else i - 1
        return remote(pb.at[i, yr], rb.at[to, yr], b_s.at[to, yr], b_r.at[to, yr],
                      ahead if i < 3 else beside)

    def last(i):
        return remote(pb.at[i, 1], ry.at[i - 3], y2_s.at[i - 3], y2_r.at[i - 3],
                      dev(z, y + 1, core))

    def every(low, high, step):
        def body(t, carry):
            step(t)
            return carry

        lax.fori_loop(low, high, body, 0)

    pairs = [(yr, r) for yr in (1, 0) for r in (0, 1)]

    @pl.when(end == 0)
    def _():
        def start(i):
            for yr, r in pairs:
                z_copy(i, yr, r).start()

        every(0, 4, start)

    for j in range(4):
        def y_start(k, j=j):
            for r in (0, 1):
                y_copy(j, k, r).start()

        every(0, early[j], y_start)

    ca, la = {}, {}

    def b_start(i):
        for yr in (1, 0):
            b_peer(i, yr).start()
            b_own(i, yr).start()

    for j in range(4):
        there = dev(chip(slots[j]), y, core + 1)
        here = dev(chip(slots[j]), y, core)
        ca[j] = remote(cols(there, 0, most * chunk), xa.at[1, j],
                       sa_s.at[j], sa_r.at[j], dev(z, y, core + 1))
        la[j] = pltpu.make_async_copy(cols(here, 0, most * chunk), xa.at[0, j], own_a.at[j])
        ca[j].start()
        la[j].start()
        if j == 0:
            every(4 - 4 * end, 6, b_start)

    for fetch in fetches:
        fetch.wait()

    def frequency(unit):
        total, value = 0, 0.0
        for b in range(lens.shape[0]):
            size = bl[b]
            inside = jnp.logical_and(unit >= total, unit < total + size)
            middle = (2 * total + size).astype(jnp.float32) * (0.5 / n)
            value = jnp.where(inside, middle, value)
            total = total + size
        return value

    beam_hot = jnp.where(
        lax.broadcasted_iota(jnp.int32, (delays.shape[0], beams), 0) == tb[...], 1.0, 0.0
    ).T.astype(jnp.bfloat16)
    step = 512 if delays.shape[1] % 512 == 0 else delays.shape[1]

    def pick_beams(i):
        span = pl.ds(pl.multiple_of(i * step, step), step)
        parts = split3(dl[:, span])
        rows = [jnp.dot(beam_hot, piece, preferred_element_type=jnp.float32) for piece in parts]
        for m, piece in enumerate(rows):
            g1[m * beams:(m + 1) * beams, span] = piece.astype(jnp.bfloat16)

    every(0, delays.shape[1] // step, pick_beams)

    def pick_elems(s):
        r, g = s % 2, s // 2
        u = end + (g // 2) * (1 - 2 * end)
        q = dev(chip(u), y + g % 2, core + r)
        row = od[q]
        hot = jnp.where(
            lax.broadcasted_iota(jnp.int32, (delays.shape[1], row.shape[1]), 0) == row, 1.0, 0.0
        ).astype(jnp.bfloat16)
        got = jnp.dot(g1[...], hot, preferred_element_type=jnp.float32)
        dt[s] = got[:beams] + got[beams:2 * beams] + got[2 * beams:]

    every(0, 6, pick_elems)
    wide = 2 * x.shape[1]

    def weigh(f, sources):
        for i, s in enumerate(sources):
            sine, cosine = sincos(f * dt[s])
            ch, cl = split2(cosine * scaling)
            sh, sl = split2(sine * scaling)
            span = slice(i * wide, (i + 1) * wide)
            wh[:beams, span] = jnp.concatenate([ch, sh], axis=1)
            wh[beams:, span] = jnp.concatenate([-sh, ch], axis=1)
            wl[:beams, span] = jnp.concatenate([cl, sl], axis=1)
            wl[beams:, span] = jnp.concatenate([-sl, cl], axis=1)

    def form(pieces):
        rows = jnp.concatenate([piece.reshape(wide, chunk) for piece in pieces], axis=0)
        xh, xl = split2(rows)
        span = slice(0, wide * len(pieces))
        dot = functools.partial(jnp.dot, preferred_element_type=jnp.float32)
        high = wh[:, span]
        return dot(high, xh) + (dot(high, xl) + dot(wl[:, span], xh))

    def a_slot(j, then):
        weigh(frequency(dev(chip(slots[j]), y, core)), (0, 1, 2, 3))
        la[j].wait()
        ca[j].wait_recv()

        def one(k):
            for r in (0, 1):
                y_copy(j, k, r).wait_recv()
            pa[j, k] = form([xa[s, j, :, :, part(k)] for s in range(4)])
            then(k)

        every(0, early[j], one)

    def join(j, to, k):
        a_wait(to, k)
        pa[j, k] += ra[to, k]

    def after0(k):
        @pl.when(end == 0)
        def _():
            a_copy(0, k).start()

    def join0(k):
        join(0, 0, k)
        a_copy(0, k).start()

    def join1(k):
        join(1, 1, k)
        a_copy(1, k).start()

    def after1(k):
        @pl.when(end == 0)
        def _():
            a_copy(1, k).start()

        @pl.when(jnp.logical_and(end == 1, k < early[0]))
        def _():
            join0(k)

    def after2(k):
        @pl.when(end == 1)
        def _():
            join(2, 3, k)

        a_copy(2, k).start()

        @pl.when(end == 1)
        def _():
            join1(k)

    def emit(got, start):
        rows = pl.ds(pl.multiple_of(start, 128), chunk)
        out[rows, 0, :] = got[:, :beams]
        out[rows, 1, :] = got[:, beams:]
        tot[...] += jnp.sum(got * got, axis=0, keepdims=True)

    def after3(k):
        @pl.when(end == 1)
        def _():
            join(3, 4, k)

        a_wait(2, k)
        emit((pa[3, k] + ra[2, k]).T, k * chunk)

    tot[...] = jnp.zeros_like(tot)
    a_slot(0, after0)

    def b_landed(i):
        for yr in (1, 0):
            b_own(i, yr).wait()
            b_peer(i, yr).wait_recv()

    every(4 - 4 * end, 6, b_landed)

    @pl.when(end == 1)
    def _():
        def z_landed(i):
            for yr, r in pairs:
                z_copy(i, yr, r).wait_recv()

        every(0, 4, z_landed)

        def b_joint(t):
            i, yr = t // 2, 1 - t % 2
            weigh(frequency(dev(chip(item_unit(i)), y + yr, core)), (0, 1, 4, 5))
            pb[i, yr] = form([xb[0, i, yr], xb[1, i, yr], xz[i, 0, yr], xz[i, 1, yr]])

        every(0, 8, b_joint)
        for i in range(3):
            for yr in (1, 0):
                b_copy(i, yr).start()

    def b_end(t):
        i, yr = 4 + t % 2, 1 - t // 2
        weigh(frequency(dev(chip(0), y + yr, core)), (0, 1))
        pb[i, yr] = form([xb[0, i, yr], xb[1, i, yr]])

    every(0, 4, b_end)
    a_slot(1, after1)

    @pl.when(end == 1)
    def _():
        for i in range(2):
            for yr in (1, 0):
                b_copy(i, yr).wait_recv()
                pb[5 - i, yr] += rb[i, yr]
                b_copy(5 - i, yr).start()
        for yr in (1, 0):
            b_copy(2, yr).wait_recv()
            pb[3, yr] += rb[2, yr]

    a_slot(2, after2)

    @pl.when(end == 1)
    def _():
        join1(most - 1)
        last(3).start()

    @pl.when(end == 0)
    def _():
        for i in (4, 5):
            for yr in (1, 0):
                b_copy(i, yr).wait_recv()
                pb[i, yr] += rb[i - 1, yr]
            last(i).start()

    a_slot(3, after3)

    def finish(i):
        last(i).wait_recv()
        emit((pb[i, 0] + ry[i - 3]).T, item_chunk(i) * chunk)

    every(4 - end, 6 - 2 * end, finish)
    pw[me] = tot[:, :beams] + tot[:, beams:]

    def p_copy(k):
        return remote(pw.at[me], pw.at[me], p_s.at[k], p_r.at[k], (me + k) % n)

    every(1, n, lambda k: p_copy(k).start())

    def last_sent(i):
        last(i).wait_send()

    every(4 - end, 6 - 2 * end, last_sent)

    def b_sent(i):
        for yr in (1, 0):
            b_peer(i, yr).wait_send()

    every(4 - 4 * end, 6, b_sent)
    for j in range(4):
        ca[j].wait_send()

        def drain(k, j=j):
            for r in (0, 1):
                y_copy(j, k, r).wait_send()
            if j < 3:
                a_copy(j, k).wait_send()

        every(0, early[j], drain)

    @pl.when(end == 0)
    def _():
        def z_sent(i):
            for yr, r in pairs:
                z_copy(i, yr, r).wait_send()

        every(0, 4, z_sent)

    @pl.when(end == 1)
    def _():
        for i in (0, 1, 2, 4, 5):
            for yr in (1, 0):
                b_copy(i, yr).wait_send()

    def p_landed(k):
        p_copy(k).wait_send()
        other = (me + n - k) % n
        remote(pw.at[other], pw.at[other], p_s.at[k], p_r.at[k], other).wait_recv()

    every(1, n, p_landed)
    power[...] = pw[...]


def conclude(n, lens, formed, power, beams, decibels, sems):
    pieces = sems.shape[0]
    rows = formed.shape[0] // pieces
    copies = []
    for i in range(pieces):
        span = pl.ds(i * rows, rows)
        copies.append(pltpu.make_async_copy(formed.at[span], beams.at[span], sems.at[i]))
        copies[-1].start()
    bands = decibels.shape[0]
    band = lax.broadcasted_iota(jnp.int32, decibels.shape, 0)
    low = jnp.zeros(decibels.shape, jnp.int32)
    size = jnp.zeros(decibels.shape, jnp.int32)
    total = 0
    for b in range(bands):
        low = jnp.where(band == b, total, low)
        size = jnp.where(band == b, lens[b], size)
        total = total + lens[b]
    high = low + size
    summed = jnp.zeros(decibels.shape, jnp.float32)
    for u in range(n):
        inside = jnp.logical_and(low <= u, u < high)
        summed = summed + jnp.where(inside, power[u], 0.0)
    mean = summed / (size.astype(jnp.float32) * formed.shape[0])
    decibels[...] = (10.0 / math.log(10.0)) * jnp.log(mean + epsilon)
    for copy in copies:
        copy.wait()


def local_ring(n, snapshots, delays, element_order, beam_table, band_len):
    local_elems = snapshots.shape[1]
    unit_cols = snapshots.shape[2] // n
    beams = beam_table.shape[0]
    most, chunk = CHUNKS - 1, unit_cols // CHUNKS
    block = (2 * beams, chunk)
    f32, sem = jnp.float32, pltpu.SemaphoreType.DMA
    raw = (2, local_elems)
    vmem, hbm, smem = (pl.BlockSpec(memory_space=m) for m in (pltpu.VMEM, pl.ANY, pltpu.SMEM))
    formed, power = pl.pallas_call(
        functools.partial(kernel, n),
        out_shape=(
            pltpu.VMEM((unit_cols, 2, beams), f32),
            pltpu.VMEM((n, 1, beams), f32),
        ),
        in_specs=[hbm] * 5,
        out_specs=(vmem, vmem),
        scratch_shapes=[
            pltpu.SMEM(band_len.shape, jnp.int32),
            pltpu.VMEM(delays.shape, f32),
            pltpu.VMEM((n, 1, local_elems), jnp.int32),
            pltpu.VMEM((1, beams), jnp.int32),
            pltpu.VMEM((3 * beams, delays.shape[1]), jnp.bfloat16),
            pltpu.VMEM((6, beams, local_elems), f32),
            pltpu.VMEM((2 * beams, 8 * local_elems), jnp.bfloat16),
            pltpu.VMEM((2 * beams, 8 * local_elems), jnp.bfloat16),
            pltpu.VMEM((4, 4) + raw + (most * chunk,), f32),
            pltpu.VMEM((2, 6, 2) + raw + (chunk,), f32),
            pltpu.VMEM((4, 2, 2) + raw + (chunk,), f32),
            pltpu.VMEM((4, most) + block, f32),
            pltpu.VMEM((6, 2) + block, f32),
            pltpu.VMEM((5, most) + block, f32),
            pltpu.VMEM((5, 2) + block, f32),
            pltpu.VMEM((3,) + block, f32),
            pltpu.VMEM((n, 1, beams), f32),
            pltpu.VMEM((1, 2 * beams), f32),
            sem((4,)), sem((4,)), sem((6, 2)),
            sem((4,)), sem((4,)), sem((6, 2)), sem((6, 2)),
            sem((2, 4, most)), sem((2, 4, most)), sem((4, 2, 2)), sem((4, 2, 2)),
            sem((3, most)), sem((5, most)), sem((5, 2)), sem((5, 2)),
            sem((3,)), sem((3,)),
            sem((n,)), sem((n,)),
        ],
        compiler_params=pltpu.CompilerParams(
            collective_id=0, has_side_effects=True, vmem_limit_bytes=54 * 1024 * 1024
        ),
    )(
        band_len, snapshots, delays,
        element_order.reshape(n, 1, local_elems), beam_table.reshape(1, beams),
    )
    formed = pltpu.with_memory_space_constraint(formed, pltpu.VMEM)
    power = pltpu.with_memory_space_constraint(power, pltpu.VMEM)
    return pl.pallas_call(
        functools.partial(conclude, n),
        out_shape=(
            jax.ShapeDtypeStruct((unit_cols, 2, beams), f32),
            jax.ShapeDtypeStruct((band_len.shape[0], beams), f32),
        ),
        in_specs=[smem, vmem, vmem],
        out_specs=(hbm, vmem),
        scratch_shapes=[sem((8,))],
    )(band_len, formed, power)


def fits(mesh):
    return mesh.shape["elem"] == SIDE * SIDE * RING


def steering(delays, element_order, beam_table, frequency):
    delay_rows = jnp.take(delays, beam_table, axis=0)
    delay_rows = jnp.take(delay_rows, element_order, axis=1)
    phases = 2.0 * math.pi * frequency * delay_rows
    scaling = float(delays.shape[1]) ** (-0.5)
    cosines = jnp.cos(phases) * scaling
    sines = -jnp.sin(phases) * scaling
    upper_rows = jnp.concatenate([cosines.T, sines.T], axis=1)
    lower_rows = jnp.concatenate([-sines.T, cosines.T], axis=1)
    return jnp.concatenate([upper_rows, lower_rows], axis=0)


def project(arrived, weights):
    columns = arrived.shape[2]
    stacked = arrived.reshape(2 * arrived.shape[1], columns)
    return lax.dot_general(
        stacked,
        weights,
        (((0,), (0,)), ((), ())),
        precision=lax.Precision.HIGHEST,
        preferred_element_type=jnp.float32,
    )


def local(snapshots, delays, element_order, beam_table, band_len):
    unit_count = lax.axis_size("elem")
    position = lax.axis_index("elem")
    frequency, band_size, selector = band_of(band_len, position, unit_count)
    weights = steering(delays, element_order, beam_table, frequency)
    beam_count = beam_table.shape[0]
    local_elems = snapshots.shape[1]
    unit_cols = snapshots.shape[2] // unit_count
    divided = snapshots.reshape(2, local_elems, unit_count, unit_cols)
    pieces = lax.all_to_all(divided, "elem", split_axis=2, concat_axis=1, tiled=True)
    formed = project(pieces.reshape(2, pieces.shape[1], pieces.shape[3]), weights)
    column_count = formed.shape[0]
    squares = jnp.sum(formed * formed, axis=0)
    power_mean = (squares[:beam_count] + squares[beam_count:]) / (
        band_size.astype(jnp.float32) * column_count
    )
    partial_value = selector[:, None] * power_mean[None, :]
    summed = lax.psum(partial_value, "elem")
    decibels = 10.0 * jnp.log10(summed + epsilon)
    return (formed.reshape(column_count, 2, beam_count), decibels)


def solution(mesh):
    n = mesh.shape["elem"]
    body = functools.partial(local_ring, n) if fits(mesh) else local
    return jax.shard_map(
        body,
        mesh=mesh,
        in_specs=(P(None, ("groups", "elem"), None), P(), P("groups"), P("groups"), P()),
        out_specs=(P("elem", None, "groups"), P(None, "groups")),
        check_vma=False,
    )
```

```python
import functools
import math

import jax
import jax.numpy as jnp
from jax import lax
from jax.experimental import pallas as pl
from jax.experimental.pallas import tpu as pltpu
from jax.sharding import PartitionSpec as P

epsilon = 1e-06
SIDE = 2
RING = 4
CHUNKS = 8


def band_of(band_len, position, unit_count):
    band_ends = jnp.cumsum(band_len)
    band_index = jnp.sum((band_ends <= position).astype(jnp.int32))
    selector = jnp.arange(band_len.shape[0], dtype=jnp.int32) == band_index
    band_size = jnp.sum(jnp.where(selector, band_len, 0))
    band_start = jnp.sum(jnp.where(selector, band_ends, 0)) - band_size
    frequency = (band_start.astype(jnp.float32) + 0.5 * band_size.astype(jnp.float32)) / float(
        unit_count
    )
    return (frequency, band_size, selector.astype(jnp.float32))


def sincos(turns):
    reduced = turns - jnp.floor(turns + 0.5)
    x = reduced * math.pi
    q = x * x
    sin_terms = [(-1.0) ** i / math.factorial(2 * i + 1) for i in range(7)]
    cos_terms = [(-1.0) ** i / math.factorial(2 * i) for i in range(8)]
    s = jnp.full_like(q, sin_terms[-1])
    for term in sin_terms[-2::-1]:
        s = s * q + term
    s = s * x
    c = jnp.full_like(q, cos_terms[-1])
    for term in cos_terms[-2::-1]:
        c = c * q + term
    return 2.0 * s * c, 1.0 - 2.0 * s * s


def split2(v):
    high = v.astype(jnp.bfloat16)
    return high, (v - high.astype(jnp.float32)).astype(jnp.bfloat16)


def split3(v):
    high = v.astype(jnp.bfloat16)
    rest = v - high.astype(jnp.float32)
    middle = rest.astype(jnp.bfloat16)
    return high, middle, (rest - middle.astype(jnp.float32)).astype(jnp.bfloat16)


def item_unit(i):
    return 3 - i + (i + RING) // (RING + 1) + i // (RING + 1)


def item_chunk(i):
    return CHUNKS - 2 + (i + RING) // (RING + 1) - i // (RING + 1)


def kernel(
    n, lens, x, delays, order, table, out, power,
    bl, dl, od, tb, g1, dt, wh, wl, xa, xb, xz, pa, pb, ra, rb, ry, pw, tot,
    in_s, own_a, own_b, sa_s, sa_r, sb_s, sb_r, sy_s, sy_r, sz_s, sz_r,
    a_s, a_r, b_s, b_r, y2_s, y2_r, p_s, p_r,
):
    me = lax.axis_index("elem")
    core = me % SIDE
    y = (me // SIDE) % SIDE
    z = me // (SIDE * SIDE)
    upper = z // 2
    end = z + upper * (RING - 1 - 2 * z)
    unit_cols = x.shape[2] // n
    chunk = unit_cols // CHUNKS
    most = CHUNKS - 1
    beams = table.shape[1]
    scaling = float(delays.shape[1]) ** (-0.5)
    slots = (3, 2, 1 - end, end)
    early = (most - 1, most, most - end, most - 1 + end)

    def chip(u):
        return u + upper * (RING - 1 - 2 * u)

    def dev(zz, yy, cc):
        return (zz * SIDE + yy % SIDE) * SIDE + cc % SIDE

    ahead = dev(chip(end + 1), y, core)
    beside = dev(chip(1 - end), y, core)

    barrier = pltpu.get_barrier_semaphore()

    def greet(target):
        pl.semaphore_signal(barrier, inc=1, device_id={"elem": target},
                            device_id_type=pl.DeviceIdType.MESH)

    for r in (0, 1):
        greet(dev(z, y + 1, core + r))
        greet(dev(chip(1 - end), y, core + r))
    greet(dev(z, y, core + 1))

    @pl.when(end == 1)
    def _():
        greet(ahead)

    fetches = [
        pltpu.make_async_copy(lens, bl, in_s.at[0]),
        pltpu.make_async_copy(delays, dl, in_s.at[1]),
        pltpu.make_async_copy(order, od, in_s.at[2]),
        pltpu.make_async_copy(table, tb, in_s.at[3]),
    ]
    for fetch in fetches:
        fetch.start()
    pl.semaphore_wait(barrier, 5 + end)

    def remote(src, dst, send, recv, target):
        return pltpu.make_async_remote_copy(
            src_ref=src, dst_ref=dst, send_sem=send, recv_sem=recv,
            device_id={"elem": target}, device_id_type=pl.DeviceIdType.MESH)

    def cols(unit, start, size):
        return x.at[:, :, pl.ds(pl.multiple_of(unit * unit_cols + start, 128), size)]

    def part(k):
        return pl.ds(pl.multiple_of(k * chunk, 128), chunk)

    def y_copy(j, k, r):
        return remote(
            cols(dev(chip(slots[j]), y + 1, core + r), k * chunk, chunk),
            xa.at[2 + r, j, :, :, part(k)],
            sy_s.at[r, j, k], sy_r.at[r, j, k], dev(z, y + 1, core + r))

    def late(i, yy, cc):
        return cols(dev(chip(item_unit(i)), yy, cc), item_chunk(i) * chunk, chunk)

    def z_copy(i, yr, r):
        return remote(
            late(i, y + yr, core + r), xz.at[i, r, yr],
            sz_s.at[i, r, yr], sz_r.at[i, r, yr], dev(chip(1 - end), y, core + r))

    def b_peer(i, yr):
        return remote(late(i, y + yr, core + 1), xb.at[1, i, yr],
                      sb_s.at[i, yr], sb_r.at[i, yr], dev(z, y, core + 1))

    def b_own(i, yr):
        return pltpu.make_async_copy(late(i, y + yr, core), xb.at[0, i, yr], own_b.at[i, yr])

    def a_copy(j, k):
        to = j + 3 * end if j < 2 else 2
        return remote(pa.at[j, k], ra.at[to, k], a_s.at[j, k], a_r.at[to, k],
                      ahead if j < 2 else beside)

    def a_wait(to, k):
        remote(pa.at[0, k], ra.at[to, k], a_s.at[0, k], a_r.at[to, k], beside).wait_recv()

    def b_ahead(i, yr):
        return remote(pb.at[i, yr], rb.at[i, yr], b_s.at[i, yr], b_r.at[i, yr], ahead)

    def b_back(i, yr):
        return remote(pb.at[i, yr], rb.at[i - 1, yr], b_s.at[i - 1, yr], b_r.at[i - 1, yr],
                      beside)

    def last(i):
        return remote(pb.at[i, 1], ry.at[i - 3], y2_s.at[i - 3], y2_r.at[i - 3],
                      dev(z, y + 1, core))

    def every(low, high, step):
        def body(t, carry):
            step(t)
            return carry

        lax.fori_loop(low, high, body, 0)

    pairs = [(yr, r) for yr in (1, 0) for r in (0, 1)]

    @pl.when(end == 0)
    def _():
        def start(i):
            for yr, r in pairs:
                z_copy(i, yr, r).start()

        every(0, 4, start)

    for j in range(4):
        def y_start(k, j=j):
            for r in (0, 1):
                y_copy(j, k, r).start()

        every(0, early[j], y_start)

    ca, la = {}, {}

    def b_start(i):
        for yr in (1, 0):
            b_peer(i, yr).start()
            b_own(i, yr).start()

    for j in range(4):
        there = dev(chip(slots[j]), y, core + 1)
        here = dev(chip(slots[j]), y, core)
        ca[j] = remote(cols(there, 0, most * chunk), xa.at[1, j],
                       sa_s.at[j], sa_r.at[j], dev(z, y, core + 1))
        la[j] = pltpu.make_async_copy(cols(here, 0, most * chunk), xa.at[0, j], own_a.at[j])
        ca[j].start()
        la[j].start()
        if j == 0:
            every(4 - 4 * end, 6, b_start)

    for fetch in fetches:
        fetch.wait()

    def frequency(unit):
        total, value = 0, 0.0
        for b in range(lens.shape[0]):
            size = bl[b]
            inside = jnp.logical_and(unit >= total, unit < total + size)
            middle = (2 * total + size).astype(jnp.float32) * (0.5 / n)
            value = jnp.where(inside, middle, value)
            total = total + size
        return value

    beam_hot = jnp.where(
        lax.broadcasted_iota(jnp.int32, (delays.shape[0], beams), 0) == tb[...], 1.0, 0.0
    ).T.astype(jnp.bfloat16)
    step = 512 if delays.shape[1] % 512 == 0 else delays.shape[1]

    def pick_beams(i):
        span = pl.ds(pl.multiple_of(i * step, step), step)
        parts = split3(dl[:, span])
        rows = [jnp.dot(beam_hot, piece, preferred_element_type=jnp.float32) for piece in parts]
        for m, piece in enumerate(rows):
            g1[m * beams:(m + 1) * beams, span] = piece.astype(jnp.bfloat16)

    every(0, delays.shape[1] // step, pick_beams)

    def pick_elems(s):
        r, g = s % 2, s // 2
        u = end + (g // 2) * (1 - 2 * end)
        q = dev(chip(u), y + g % 2, core + r)
        row = od[q]
        hot = jnp.where(
            lax.broadcasted_iota(jnp.int32, (delays.shape[1], row.shape[1]), 0) == row, 1.0, 0.0
        ).astype(jnp.bfloat16)
        got = jnp.dot(g1[...], hot, preferred_element_type=jnp.float32)
        dt[s] = got[:beams] + got[beams:2 * beams] + got[2 * beams:]

    every(0, 6, pick_elems)
    wide = 2 * x.shape[1]

    def weigh(f, sources):
        for i, s in enumerate(sources):
            sine, cosine = sincos(f * dt[s])
            ch, cl = split2(cosine * scaling)
            sh, sl = split2(sine * scaling)
            span = slice(i * wide, (i + 1) * wide)
            wh[:beams, span] = jnp.concatenate([ch, sh], axis=1)
            wh[beams:, span] = jnp.concatenate([-sh, ch], axis=1)
            wl[:beams, span] = jnp.concatenate([cl, sl], axis=1)
            wl[beams:, span] = jnp.concatenate([-sl, cl], axis=1)

    def form(pieces):
        rows = jnp.concatenate([piece.reshape(wide, chunk) for piece in pieces], axis=0)
        xh, xl = split2(rows)
        span = slice(0, wide * len(pieces))
        dot = functools.partial(jnp.dot, preferred_element_type=jnp.float32)
        high = wh[:, span]
        return dot(high, xh) + (dot(high, xl) + dot(wl[:, span], xh))

    def a_slot(j, then):
        weigh(frequency(dev(chip(slots[j]), y, core)), (0, 1, 2, 3))
        la[j].wait()
        ca[j].wait_recv()

        def one(k):
            for r in (0, 1):
                y_copy(j, k, r).wait_recv()
            pa[j, k] = form([xa[s, j, :, :, part(k)] for s in range(4)])
            then(k)

        every(0, early[j], one)

    def join(j, to, k):
        a_wait(to, k)
        pa[j, k] += ra[to, k]

    def after0(k):
        @pl.when(end == 0)
        def _():
            a_copy(0, k).start()

    def join0(k):
        join(0, 0, k)
        a_copy(0, k).start()

    def join1(k):
        join(1, 1, k)
        a_copy(1, k).start()

    def after1(k):
        @pl.when(end == 0)
        def _():
            a_copy(1, k).start()

        @pl.when(jnp.logical_and(end == 1, k < early[0]))
        def _():
            join0(k)

    def after2(k):
        @pl.when(end == 1)
        def _():
            join(2, 3, k)

        a_copy(2, k).start()

        @pl.when(end == 1)
        def _():
            join1(k)

    def emit(got, start):
        rows = pl.ds(pl.multiple_of(start, 128), chunk)
        out[rows, 0, :] = got[:, :beams]
        out[rows, 1, :] = got[:, beams:]
        tot[...] += jnp.sum(got * got, axis=0, keepdims=True)

    def after3(k):
        @pl.when(end == 1)
        def _():
            join(3, 4, k)

        a_wait(2, k)
        emit((pa[3, k] + ra[2, k]).T, k * chunk)

    tot[...] = jnp.zeros_like(tot)

    def b_landed(i, yr):
        b_own(i, yr).wait()
        b_peer(i, yr).wait_recv()

    def b_joint(i, yr):
        for r in (0, 1):
            z_copy(i, yr, r).wait_recv()
        b_landed(i, yr)
        weigh(frequency(dev(chip(item_unit(i)), y + yr, core)), (0, 1, 4, 5))
        pb[i, yr] = form([xb[0, i, yr], xb[1, i, yr], xz[i, 0, yr], xz[i, 1, yr]])

    @pl.when(end == 1)
    def _():
        def b_first(t):
            i, yr = t // 2, 1 - t % 2
            b_joint(i, yr)
            b_ahead(i, yr).start()

        every(0, 6, b_first)

    a_slot(0, after0)

    def b_end(t):
        i, yr = 4 + t % 2, 1 - t // 2
        b_landed(i, yr)
        weigh(frequency(dev(chip(0), y + yr, core)), (0, 1))
        pb[i, yr] = form([xb[0, i, yr], xb[1, i, yr]])

    every(0, 4, b_end)
    a_slot(1, after1)

    @pl.when(end == 1)
    def _():
        for i in range(2):
            for yr in (1, 0):
                b_ahead(i, yr).wait_recv()
                pb[5 - i, yr] += rb[i, yr]
                b_back(5 - i, yr).start()

        def b_home(t):
            yr = 1 - t
            b_joint(3, yr)
            b_ahead(2, yr).wait_recv()
            pb[3, yr] += rb[2, yr]

        every(0, 2, b_home)

    a_slot(2, after2)

    @pl.when(end == 1)
    def _():
        join1(most - 1)
        last(3).start()

    @pl.when(end == 0)
    def _():
        for i in (4, 5):
            for yr in (1, 0):
                b_back(i, yr).wait_recv()
                pb[i, yr] += rb[i - 1, yr]
            last(i).start()

    a_slot(3, after3)

    def finish(i):
        last(i).wait_recv()
        emit((pb[i, 0] + ry[i - 3]).T, item_chunk(i) * chunk)

    every(4 - end, 6 - 2 * end, finish)
    pw[me] = tot[:, :beams] + tot[:, beams:]

    def p_copy(k):
        return remote(pw.at[me], pw.at[me], p_s.at[k], p_r.at[k], (me + k) % n)

    every(1, n, lambda k: p_copy(k).start())

    def last_sent(i):
        last(i).wait_send()

    every(4 - end, 6 - 2 * end, last_sent)

    def b_sent(i):
        for yr in (1, 0):
            b_peer(i, yr).wait_send()

    every(4 - 4 * end, 6, b_sent)
    for j in range(4):
        ca[j].wait_send()

        def drain(k, j=j):
            for r in (0, 1):
                y_copy(j, k, r).wait_send()
            if j < 3:
                a_copy(j, k).wait_send()

        every(0, early[j], drain)

    @pl.when(end == 0)
    def _():
        def z_sent(i):
            for yr, r in pairs:
                z_copy(i, yr, r).wait_send()

        every(0, 4, z_sent)

    @pl.when(end == 1)
    def _():
        for yr in (1, 0):
            for i in range(3):
                b_ahead(i, yr).wait_send()
            for i in (4, 5):
                b_back(i, yr).wait_send()

    def p_landed(k):
        p_copy(k).wait_send()
        other = (me + n - k) % n
        remote(pw.at[other], pw.at[other], p_s.at[k], p_r.at[k], other).wait_recv()

    every(1, n, p_landed)
    power[...] = pw[...]


def conclude(n, lens, formed, power, beams, decibels, sems):
    pieces = sems.shape[0]
    rows = formed.shape[0] // pieces
    copies = []
    for i in range(pieces):
        span = pl.ds(i * rows, rows)
        copies.append(pltpu.make_async_copy(formed.at[span], beams.at[span], sems.at[i]))
        copies[-1].start()
    bands = decibels.shape[0]
    band = lax.broadcasted_iota(jnp.int32, decibels.shape, 0)
    low = jnp.zeros(decibels.shape, jnp.int32)
    size = jnp.zeros(decibels.shape, jnp.int32)
    total = 0
    for b in range(bands):
        low = jnp.where(band == b, total, low)
        size = jnp.where(band == b, lens[b], size)
        total = total + lens[b]
    high = low + size
    summed = jnp.zeros(decibels.shape, jnp.float32)
    for u in range(n):
        inside = jnp.logical_and(low <= u, u < high)
        summed = summed + jnp.where(inside, power[u], 0.0)
    mean = summed / (size.astype(jnp.float32) * formed.shape[0])
    decibels[...] = (10.0 / math.log(10.0)) * jnp.log(mean + epsilon)
    for copy in copies:
        copy.wait()


def local_ring(n, snapshots, delays, element_order, beam_table, band_len):
    local_elems = snapshots.shape[1]
    unit_cols = snapshots.shape[2] // n
    beams = beam_table.shape[0]
    most, chunk = CHUNKS - 1, unit_cols // CHUNKS
    block = (2 * beams, chunk)
    f32, sem = jnp.float32, pltpu.SemaphoreType.DMA
    raw = (2, local_elems)
    vmem, hbm, smem = (pl.BlockSpec(memory_space=m) for m in (pltpu.VMEM, pl.ANY, pltpu.SMEM))
    formed, power = pl.pallas_call(
        functools.partial(kernel, n),
        out_shape=(
            pltpu.VMEM((unit_cols, 2, beams), f32),
            pltpu.VMEM((n, 1, beams), f32),
        ),
        in_specs=[hbm] * 5,
        out_specs=(vmem, vmem),
        scratch_shapes=[
            pltpu.SMEM(band_len.shape, jnp.int32),
            pltpu.VMEM(delays.shape, f32),
            pltpu.VMEM((n, 1, local_elems), jnp.int32),
            pltpu.VMEM((1, beams), jnp.int32),
            pltpu.VMEM((3 * beams, delays.shape[1]), jnp.bfloat16),
            pltpu.VMEM((6, beams, local_elems), f32),
            pltpu.VMEM((2 * beams, 8 * local_elems), jnp.bfloat16),
            pltpu.VMEM((2 * beams, 8 * local_elems), jnp.bfloat16),
            pltpu.VMEM((4, 4) + raw + (most * chunk,), f32),
            pltpu.VMEM((2, 6, 2) + raw + (chunk,), f32),
            pltpu.VMEM((4, 2, 2) + raw + (chunk,), f32),
            pltpu.VMEM((4, most) + block, f32),
            pltpu.VMEM((6, 2) + block, f32),
            pltpu.VMEM((5, most) + block, f32),
            pltpu.VMEM((5, 2) + block, f32),
            pltpu.VMEM((3,) + block, f32),
            pltpu.VMEM((n, 1, beams), f32),
            pltpu.VMEM((1, 2 * beams), f32),
            sem((4,)), sem((4,)), sem((6, 2)),
            sem((4,)), sem((4,)), sem((6, 2)), sem((6, 2)),
            sem((2, 4, most)), sem((2, 4, most)), sem((4, 2, 2)), sem((4, 2, 2)),
            sem((3, most)), sem((5, most)), sem((5, 2)), sem((5, 2)),
            sem((3,)), sem((3,)),
            sem((n,)), sem((n,)),
        ],
        compiler_params=pltpu.CompilerParams(
            collective_id=0, has_side_effects=True, vmem_limit_bytes=54 * 1024 * 1024
        ),
    )(
        band_len, snapshots, delays,
        element_order.reshape(n, 1, local_elems), beam_table.reshape(1, beams),
    )
    formed = pltpu.with_memory_space_constraint(formed, pltpu.VMEM)
    power = pltpu.with_memory_space_constraint(power, pltpu.VMEM)
    return pl.pallas_call(
        functools.partial(conclude, n),
        out_shape=(
            jax.ShapeDtypeStruct((unit_cols, 2, beams), f32),
            jax.ShapeDtypeStruct((band_len.shape[0], beams), f32),
        ),
        in_specs=[smem, vmem, vmem],
        out_specs=(hbm, vmem),
        scratch_shapes=[sem((8,))],
    )(band_len, formed, power)


def fits(mesh):
    return mesh.shape["elem"] == SIDE * SIDE * RING


def steering(delays, element_order, beam_table, frequency):
    delay_rows = jnp.take(delays, beam_table, axis=0)
    delay_rows = jnp.take(delay_rows, element_order, axis=1)
    phases = 2.0 * math.pi * frequency * delay_rows
    scaling = float(delays.shape[1]) ** (-0.5)
    cosines = jnp.cos(phases) * scaling
    sines = -jnp.sin(phases) * scaling
    upper_rows = jnp.concatenate([cosines.T, sines.T], axis=1)
    lower_rows = jnp.concatenate([-sines.T, cosines.T], axis=1)
    return jnp.concatenate([upper_rows, lower_rows], axis=0)


def project(arrived, weights):
    columns = arrived.shape[2]
    stacked = arrived.reshape(2 * arrived.shape[1], columns)
    return lax.dot_general(
        stacked,
        weights,
        (((0,), (0,)), ((), ())),
        precision=lax.Precision.HIGHEST,
        preferred_element_type=jnp.float32,
    )


def local(snapshots, delays, element_order, beam_table, band_len):
    unit_count = lax.axis_size("elem")
    position = lax.axis_index("elem")
    frequency, band_size, selector = band_of(band_len, position, unit_count)
    weights = steering(delays, element_order, beam_table, frequency)
    beam_count = beam_table.shape[0]
    local_elems = snapshots.shape[1]
    unit_cols = snapshots.shape[2] // unit_count
    divided = snapshots.reshape(2, local_elems, unit_count, unit_cols)
    pieces = lax.all_to_all(divided, "elem", split_axis=2, concat_axis=1, tiled=True)
    formed = project(pieces.reshape(2, pieces.shape[1], pieces.shape[3]), weights)
    column_count = formed.shape[0]
    squares = jnp.sum(formed * formed, axis=0)
    power_mean = (squares[:beam_count] + squares[beam_count:]) / (
        band_size.astype(jnp.float32) * column_count
    )
    partial_value = selector[:, None] * power_mean[None, :]
    summed = lax.psum(partial_value, "elem")
    decibels = 10.0 * jnp.log10(summed + epsilon)
    return (formed.reshape(column_count, 2, beam_count), decibels)


def solution(mesh):
    n = mesh.shape["elem"]
    body = functools.partial(local_ring, n) if fits(mesh) else local
    return jax.shard_map(
        body,
        mesh=mesh,
        in_specs=(P(None, ("groups", "elem"), None), P(), P("groups"), P("groups"), P()),
        out_specs=(P("elem", None, "groups"), P(None, "groups")),
        check_vma=False,
    )
```

```python
import functools
import math

import jax
import jax.numpy as jnp
from jax import lax
from jax.experimental import pallas as pl
from jax.experimental.pallas import tpu as pltpu
from jax.sharding import PartitionSpec as P

epsilon = 1e-06
SIDE = 2
RING = 4
CHUNKS = 8


def band_of(band_len, position, unit_count):
    band_ends = jnp.cumsum(band_len)
    band_index = jnp.sum((band_ends <= position).astype(jnp.int32))
    selector = jnp.arange(band_len.shape[0], dtype=jnp.int32) == band_index
    band_size = jnp.sum(jnp.where(selector, band_len, 0))
    band_start = jnp.sum(jnp.where(selector, band_ends, 0)) - band_size
    frequency = (band_start.astype(jnp.float32) + 0.5 * band_size.astype(jnp.float32)) / float(
        unit_count
    )
    return (frequency, band_size, selector.astype(jnp.float32))


def sincos(turns):
    reduced = turns - jnp.floor(turns + 0.5)
    x = reduced * math.pi
    q = x * x
    sin_terms = [(-1.0) ** i / math.factorial(2 * i + 1) for i in range(7)]
    cos_terms = [(-1.0) ** i / math.factorial(2 * i) for i in range(8)]
    s = jnp.full_like(q, sin_terms[-1])
    for term in sin_terms[-2::-1]:
        s = s * q + term
    s = s * x
    c = jnp.full_like(q, cos_terms[-1])
    for term in cos_terms[-2::-1]:
        c = c * q + term
    return 2.0 * s * c, 1.0 - 2.0 * s * s


def split2(v):
    high = v.astype(jnp.bfloat16)
    return high, (v - high.astype(jnp.float32)).astype(jnp.bfloat16)


def split3(v):
    high = v.astype(jnp.bfloat16)
    rest = v - high.astype(jnp.float32)
    middle = rest.astype(jnp.bfloat16)
    return high, middle, (rest - middle.astype(jnp.float32)).astype(jnp.bfloat16)


def item_unit(i):
    return 3 - i + (i + RING) // (RING + 1) + i // (RING + 1)


def item_chunk(i):
    return CHUNKS - 2 + (i + RING) // (RING + 1) - i // (RING + 1)


def kernel(
    n, lens, x, delays, order, table, out, power, bands,
    bl, dl, od, tb, g1, dt, wh, wl, xa, xb, xz, pa, pb, ra, rb, ry, pw, tot,
    in_s, own_a, own_b, sa_s, sa_r, sb_s, sb_r, sy_s, sy_r, sz_s, sz_r,
    a_s, a_r, b_s, b_r, y2_s, y2_r, p_s, p_r,
):
    me = lax.axis_index("elem")
    core = me % SIDE
    y = (me // SIDE) % SIDE
    z = me // (SIDE * SIDE)
    upper = z // 2
    end = z + upper * (RING - 1 - 2 * z)
    unit_cols = x.shape[2] // n
    chunk = unit_cols // CHUNKS
    most = CHUNKS - 1
    beams = table.shape[1]
    scaling = float(delays.shape[1]) ** (-0.5)
    slots = (3, 2, 1 - end, end)
    early = (most - 1, most, most - end, most - 1 + end)

    def chip(u):
        return u + upper * (RING - 1 - 2 * u)

    def dev(zz, yy, cc):
        return (zz * SIDE + yy % SIDE) * SIDE + cc % SIDE

    ahead = dev(chip(end + 1), y, core)
    beside = dev(chip(1 - end), y, core)

    barrier = pltpu.get_barrier_semaphore()

    def greet(target):
        pl.semaphore_signal(barrier, inc=1, device_id={"elem": target},
                            device_id_type=pl.DeviceIdType.MESH)

    for r in (0, 1):
        greet(dev(z, y + 1, core + r))
        greet(dev(chip(1 - end), y, core + r))
    greet(dev(z, y, core + 1))

    @pl.when(end == 1)
    def _():
        greet(ahead)

    fetches = [
        pltpu.make_async_copy(lens, bl, in_s.at[0]),
        pltpu.make_async_copy(delays, dl, in_s.at[1]),
        pltpu.make_async_copy(order, od, in_s.at[2]),
        pltpu.make_async_copy(table, tb, in_s.at[3]),
    ]
    for fetch in fetches:
        fetch.start()
    pl.semaphore_wait(barrier, 5 + end)

    def remote(src, dst, send, recv, target):
        return pltpu.make_async_remote_copy(
            src_ref=src, dst_ref=dst, send_sem=send, recv_sem=recv,
            device_id={"elem": target}, device_id_type=pl.DeviceIdType.MESH)

    def cols(unit, start, size):
        return x.at[:, :, pl.ds(pl.multiple_of(unit * unit_cols + start, 128), size)]

    def part(k):
        return pl.ds(pl.multiple_of(k * chunk, 128), chunk)

    def y_copy(j, k, r):
        return remote(
            cols(dev(chip(slots[j]), y + 1, core + r), k * chunk, chunk),
            xa.at[2 + r, j, :, :, part(k)],
            sy_s.at[r, j, k], sy_r.at[r, j, k], dev(z, y + 1, core + r))

    def late(i, yy, cc):
        return cols(dev(chip(item_unit(i)), yy, cc), item_chunk(i) * chunk, chunk)

    def z_copy(i, yr, r):
        return remote(
            late(i, y + yr, core + r), xz.at[i, r, yr],
            sz_s.at[i, r, yr], sz_r.at[i, r, yr], dev(chip(1 - end), y, core + r))

    def b_peer(i, yr):
        return remote(late(i, y + yr, core + 1), xb.at[1, i, yr],
                      sb_s.at[i, yr], sb_r.at[i, yr], dev(z, y, core + 1))

    def b_own(i, yr):
        return pltpu.make_async_copy(late(i, y + yr, core), xb.at[0, i, yr], own_b.at[i, yr])

    def a_copy(j, k):
        to = j + 3 * end if j < 2 else 2
        return remote(pa.at[j, k], ra.at[to, k], a_s.at[j, k], a_r.at[to, k],
                      ahead if j < 2 else beside)

    def a_wait(to, k):
        remote(pa.at[0, k], ra.at[to, k], a_s.at[0, k], a_r.at[to, k], beside).wait_recv()

    def b_ahead(i, yr):
        return remote(pb.at[i, yr], rb.at[i, yr], b_s.at[i, yr], b_r.at[i, yr], ahead)

    def b_back(i, yr):
        return remote(pb.at[i, yr], rb.at[i - 1, yr], b_s.at[i - 1, yr], b_r.at[i - 1, yr],
                      beside)

    def last(i):
        return remote(pb.at[i, 1], ry.at[i - 3], y2_s.at[i - 3], y2_r.at[i - 3],
                      dev(z, y + 1, core))

    def every(low, high, step):
        def body(t, carry):
            step(t)
            return carry

        lax.fori_loop(low, high, body, 0)

    pairs = [(yr, r) for yr in (1, 0) for r in (0, 1)]

    def y_start(j):
        def start(k):
            for r in (0, 1):
                y_copy(j, k, r).start()

        every(0, early[j], start)

    @pl.when(end == 0)
    def _():
        for r in (0, 1):
            z_copy(0, 1, r).start()

    y_start(0)

    @pl.when(end == 0)
    def _():
        def start(t):
            for r in (0, 1):
                z_copy(t // 2, 1 - t % 2, r).start()

        every(1, 8, start)

    for j in (1, 2, 3):
        y_start(j)

    ca, la = {}, {}

    def b_start(i):
        for yr in (1, 0):
            b_peer(i, yr).start()
            b_own(i, yr).start()

    for j in range(4):
        there = dev(chip(slots[j]), y, core + 1)
        here = dev(chip(slots[j]), y, core)
        ca[j] = remote(cols(there, 0, most * chunk), xa.at[1, j],
                       sa_s.at[j], sa_r.at[j], dev(z, y, core + 1))
        la[j] = pltpu.make_async_copy(cols(here, 0, most * chunk), xa.at[0, j], own_a.at[j])
        ca[j].start()
        la[j].start()
        if j == 0:
            every(4 - 4 * end, 6, b_start)

    for fetch in fetches:
        fetch.wait()

    def frequency(unit):
        total, value = 0, 0.0
        for b in range(lens.shape[0]):
            size = bl[b]
            inside = jnp.logical_and(unit >= total, unit < total + size)
            middle = (2 * total + size).astype(jnp.float32) * (0.5 / n)
            value = jnp.where(inside, middle, value)
            total = total + size
        return value

    band = lax.broadcasted_iota(jnp.int32, bands.shape[1:], 0)
    total = 0
    for b in range(lens.shape[0]):
        bands[0] = jnp.where(band == b, total, bands[0] if b else 0)
        bands[1] = jnp.where(band == b, bl[b], bands[1] if b else 0)
        total = total + bl[b]

    beam_hot = jnp.where(
        lax.broadcasted_iota(jnp.int32, (delays.shape[0], beams), 0) == tb[...], 1.0, 0.0
    ).T.astype(jnp.bfloat16)
    step = 512 if delays.shape[1] % 512 == 0 else delays.shape[1]

    def pick_beams(i):
        span = pl.ds(pl.multiple_of(i * step, step), step)
        parts = split3(dl[:, span])
        rows = [jnp.dot(beam_hot, piece, preferred_element_type=jnp.float32) for piece in parts]
        for m, piece in enumerate(rows):
            g1[m * beams:(m + 1) * beams, span] = piece.astype(jnp.bfloat16)

    every(0, delays.shape[1] // step, pick_beams)

    def pick_elems(s):
        r, g = s % 2, s // 2
        u = end + (g // 2) * (1 - 2 * end)
        q = dev(chip(u), y + g % 2, core + r)
        row = od[q]
        hot = jnp.where(
            lax.broadcasted_iota(jnp.int32, (delays.shape[1], row.shape[1]), 0) == row, 1.0, 0.0
        ).astype(jnp.bfloat16)
        got = jnp.dot(g1[...], hot, preferred_element_type=jnp.float32)
        dt[s] = got[:beams] + got[beams:2 * beams] + got[2 * beams:]

    every(0, 6, pick_elems)
    wide = 2 * x.shape[1]

    def weigh(f, sources):
        for i, s in enumerate(sources):
            sine, cosine = sincos(f * dt[s])
            ch, cl = split2(cosine * scaling)
            sh, sl = split2(sine * scaling)
            span = slice(i * wide, (i + 1) * wide)
            wh[:beams, span] = jnp.concatenate([ch, sh], axis=1)
            wh[beams:, span] = jnp.concatenate([-sh, ch], axis=1)
            wl[:beams, span] = jnp.concatenate([cl, sl], axis=1)
            wl[beams:, span] = jnp.concatenate([-sl, cl], axis=1)

    def form(pieces):
        rows = jnp.concatenate([piece.reshape(wide, chunk) for piece in pieces], axis=0)
        xh, xl = split2(rows)
        span = slice(0, wide * len(pieces))
        dot = functools.partial(jnp.dot, preferred_element_type=jnp.float32)
        high = wh[:, span]
        return dot(high, xh) + (dot(high, xl) + dot(wl[:, span], xh))

    def a_slot(j, then, pause=None):
        weigh(frequency(dev(chip(slots[j]), y, core)), (0, 1, 2, 3))
        la[j].wait()
        ca[j].wait_recv()

        def one(k):
            for r in (0, 1):
                y_copy(j, k, r).wait_recv()
            pa[j, k] = form([xa[s, j, :, :, part(k)] for s in range(4)])
            then(k)

        if pause is None:
            every(0, early[j], one)
        else:
            every(0, early[j] - 1, one)
            pause()
            one(early[j] - 1)

    def join(j, to, k):
        a_wait(to, k)
        pa[j, k] += ra[to, k]

    def after0(k):
        @pl.when(end == 0)
        def _():
            a_copy(0, k).start()

    def join0(k):
        join(0, 0, k)
        a_copy(0, k).start()

    def join1(k):
        join(1, 1, k)
        a_copy(1, k).start()

    def after1(k):
        @pl.when(end == 0)
        def _():
            a_copy(1, k).start()

        @pl.when(jnp.logical_and(end == 1, k < early[0]))
        def _():
            join0(k)

    def after2(k):
        @pl.when(end == 1)
        def _():
            join(2, 3, k)

        a_copy(2, k).start()

        @pl.when(end == 1)
        def _():
            join1(k)

    def emit(got, start):
        rows = pl.ds(pl.multiple_of(start, 128), chunk)
        out[rows, 0, :] = got[:, :beams]
        out[rows, 1, :] = got[:, beams:]
        tot[...] += jnp.sum(got * got, axis=0, keepdims=True)

    def after3(k):
        @pl.when(end == 1)
        def _():
            join(3, 4, k)

        a_wait(2, k)
        emit((pa[3, k] + ra[2, k]).T, k * chunk)

    tot[...] = jnp.zeros_like(tot)

    def b_landed(i, yr):
        b_own(i, yr).wait()
        b_peer(i, yr).wait_recv()

    def b_joint(i, yr):
        for r in (0, 1):
            z_copy(i, yr, r).wait_recv()
        b_landed(i, yr)
        weigh(frequency(dev(chip(item_unit(i)), y + yr, core)), (0, 1, 4, 5))
        pb[i, yr] = form([xb[0, i, yr], xb[1, i, yr], xz[i, 0, yr], xz[i, 1, yr]])

    @pl.when(end == 1)
    def _():
        def b_first(t):
            i, yr = t // 2, 1 - t % 2
            b_joint(i, yr)
            b_ahead(i, yr).start()

        every(0, 6, b_first)

    a_slot(0, after0)

    def b_end(t):
        i, yr = 4 + t % 2, 1 - t // 2
        b_landed(i, yr)
        weigh(frequency(dev(chip(0), y + yr, core)), (0, 1))
        pb[i, yr] = form([xb[0, i, yr], xb[1, i, yr]])

    every(0, 4, b_end)
    a_slot(1, after1)

    @pl.when(end == 1)
    def _():
        for i in range(2):
            for yr in (1, 0):
                b_ahead(i, yr).wait_recv()
                pb[5 - i, yr] += rb[i, yr]
                b_back(5 - i, yr).start()

        def b_home(t):
            yr = 1 - t
            b_joint(3, yr)
            b_ahead(2, yr).wait_recv()
            pb[3, yr] += rb[2, yr]

        every(0, 2, b_home)

    a_slot(2, after2)

    @pl.when(end == 1)
    def _():
        join1(most - 1)
        last(3).start()

    @pl.when(end == 0)
    def _():
        for i in (4, 5):
            for yr in (1, 0):
                b_back(i, yr).wait_recv()
                pb[i, yr] += rb[i - 1, yr]
            last(i).start()

    def finish(i):
        last(i).wait_recv()
        emit((pb[i, 0] + ry[i - 3]).T, item_chunk(i) * chunk)

    a_slot(3, after3, lambda: every(3, 3 + end, finish))
    every(4, 6 - 2 * end, finish)
    pw[me] = tot[:, :beams] + tot[:, beams:]

    def p_copy(target):
        return remote(pw.at[me], pw.at[me], p_s.at[target], p_r.at[me], target)

    def p_far(t):
        p_copy(dev(chip(3 - t // (SIDE * SIDE)), y + 1 + t // SIDE, core + t)).start()

    others = 3 - end
    every(0, others * SIDE * SIDE, p_far)

    @pl.when(end == 1)
    def _():
        for t in range(SIDE * SIDE):
            p_copy(dev(chip(0), y + 1 + t // SIDE, core + t)).start()

    for t in range(SIDE * SIDE - 1):
        p_copy(dev(z, y + 1 + t // SIDE, core + t + t // SIDE)).start()

    def last_sent(i):
        last(i).wait_send()

    every(4 - end, 6 - 2 * end, last_sent)

    def b_sent(i):
        for yr in (1, 0):
            b_peer(i, yr).wait_send()

    every(4 - 4 * end, 6, b_sent)
    for j in range(4):
        ca[j].wait_send()

        def drain(k, j=j):
            for r in (0, 1):
                y_copy(j, k, r).wait_send()
            if j < 3:
                a_copy(j, k).wait_send()

        every(0, early[j], drain)

    @pl.when(end == 0)
    def _():
        def z_sent(i):
            for yr, r in pairs:
                z_copy(i, yr, r).wait_send()

        every(0, 4, z_sent)

    @pl.when(end == 1)
    def _():
        for yr in (1, 0):
            for i in range(3):
                b_ahead(i, yr).wait_send()
            for i in (4, 5):
                b_back(i, yr).wait_send()

    def p_landed(k):
        other = (me + k) % n
        p_copy(other).wait_send()
        remote(pw.at[other], pw.at[other], p_s.at[other], p_r.at[other], other).wait_recv()

    every(1, n, p_landed)
    power[...] = pw[...]


def conclude(n, formed, power, bands, beams, decibels, level, sems):
    pieces = sems.shape[0] - 1
    rows = formed.shape[0] // pieces
    copies = []
    for i in range(pieces):
        span = pl.ds(i * rows, rows)
        copies.append(pltpu.make_async_copy(formed.at[span], beams.at[span], sems.at[i]))
        copies[-1].start()
    low, size = bands[0], bands[1]
    high = low + size
    summed = jnp.zeros(level.shape, jnp.float32)
    for u in range(n):
        inside = jnp.logical_and(low <= u, u < high)
        summed = summed + jnp.where(inside, power[u], 0.0)
    mean = summed / (size.astype(jnp.float32) * formed.shape[0])
    level[...] = (10.0 / math.log(10.0)) * jnp.log(mean + epsilon)
    copies.append(pltpu.make_async_copy(level, decibels, sems.at[pieces]))
    copies[-1].start()
    for copy in copies:
        copy.wait()


def local_ring(n, snapshots, delays, element_order, beam_table, band_len):
    local_elems = snapshots.shape[1]
    unit_cols = snapshots.shape[2] // n
    beams = beam_table.shape[0]
    most, chunk = CHUNKS - 1, unit_cols // CHUNKS
    block = (2 * beams, chunk)
    f32, sem = jnp.float32, pltpu.SemaphoreType.DMA
    raw = (2, local_elems)
    vmem, hbm = (pl.BlockSpec(memory_space=m) for m in (pltpu.VMEM, pl.ANY))
    band_shape = (band_len.shape[0], beams)
    formed, power, bands = pl.pallas_call(
        functools.partial(kernel, n),
        out_shape=(
            pltpu.VMEM((unit_cols, 2, beams), f32),
            pltpu.VMEM((n, 1, beams), f32),
            pltpu.VMEM((2,) + band_shape, jnp.int32),
        ),
        in_specs=[hbm] * 5,
        out_specs=(vmem, vmem, vmem),
        scratch_shapes=[
            pltpu.SMEM(band_len.shape, jnp.int32),
            pltpu.VMEM(delays.shape, f32),
            pltpu.VMEM((n, 1, local_elems), jnp.int32),
            pltpu.VMEM((1, beams), jnp.int32),
            pltpu.VMEM((3 * beams, delays.shape[1]), jnp.bfloat16),
            pltpu.VMEM((6, beams, local_elems), f32),
            pltpu.VMEM((2 * beams, 8 * local_elems), jnp.bfloat16),
            pltpu.VMEM((2 * beams, 8 * local_elems), jnp.bfloat16),
            pltpu.VMEM((4, 4) + raw + (most * chunk,), f32),
            pltpu.VMEM((2, 6, 2) + raw + (chunk,), f32),
            pltpu.VMEM((4, 2, 2) + raw + (chunk,), f32),
            pltpu.VMEM((4, most) + block, f32),
            pltpu.VMEM((6, 2) + block, f32),
            pltpu.VMEM((5, most) + block, f32),
            pltpu.VMEM((5, 2) + block, f32),
            pltpu.VMEM((3,) + block, f32),
            pltpu.VMEM((n, 1, beams), f32),
            pltpu.VMEM((1, 2 * beams), f32),
            sem((4,)), sem((4,)), sem((6, 2)),
            sem((4,)), sem((4,)), sem((6, 2)), sem((6, 2)),
            sem((2, 4, most)), sem((2, 4, most)), sem((4, 2, 2)), sem((4, 2, 2)),
            sem((3, most)), sem((5, most)), sem((5, 2)), sem((5, 2)),
            sem((3,)), sem((3,)),
            sem((n,)), sem((n,)),
        ],
        compiler_params=pltpu.CompilerParams(
            collective_id=0, has_side_effects=True, vmem_limit_bytes=54 * 1024 * 1024
        ),
    )(
        band_len, snapshots, delays,
        element_order.reshape(n, 1, local_elems), beam_table.reshape(1, beams),
    )
    parts = [pltpu.with_memory_space_constraint(v, pltpu.VMEM) for v in (formed, power, bands)]
    return pl.pallas_call(
        functools.partial(conclude, n),
        out_shape=(
            jax.ShapeDtypeStruct((unit_cols, 2, beams), f32),
            jax.ShapeDtypeStruct(band_shape, f32),
        ),
        in_specs=[vmem] * 3,
        out_specs=(hbm, hbm),
        scratch_shapes=[pltpu.VMEM(band_shape, f32), sem((9,))],
    )(*parts)


def fits(mesh):
    return mesh.shape["elem"] == SIDE * SIDE * RING


def steering(delays, element_order, beam_table, frequency):
    delay_rows = jnp.take(delays, beam_table, axis=0)
    delay_rows = jnp.take(delay_rows, element_order, axis=1)
    phases = 2.0 * math.pi * frequency * delay_rows
    scaling = float(delays.shape[1]) ** (-0.5)
    cosines = jnp.cos(phases) * scaling
    sines = -jnp.sin(phases) * scaling
    upper_rows = jnp.concatenate([cosines.T, sines.T], axis=1)
    lower_rows = jnp.concatenate([-sines.T, cosines.T], axis=1)
    return jnp.concatenate([upper_rows, lower_rows], axis=0)


def project(arrived, weights):
    columns = arrived.shape[2]
    stacked = arrived.reshape(2 * arrived.shape[1], columns)
    return lax.dot_general(
        stacked,
        weights,
        (((0,), (0,)), ((), ())),
        precision=lax.Precision.HIGHEST,
        preferred_element_type=jnp.float32,
    )


def local(snapshots, delays, element_order, beam_table, band_len):
    unit_count = lax.axis_size("elem")
    position = lax.axis_index("elem")
    frequency, band_size, selector = band_of(band_len, position, unit_count)
    weights = steering(delays, element_order, beam_table, frequency)
    beam_count = beam_table.shape[0]
    local_elems = snapshots.shape[1]
    unit_cols = snapshots.shape[2] // unit_count
    divided = snapshots.reshape(2, local_elems, unit_count, unit_cols)
    pieces = lax.all_to_all(divided, "elem", split_axis=2, concat_axis=1, tiled=True)
    formed = project(pieces.reshape(2, pieces.shape[1], pieces.shape[3]), weights)
    column_count = formed.shape[0]
    squares = jnp.sum(formed * formed, axis=0)
    power_mean = (squares[:beam_count] + squares[beam_count:]) / (
        band_size.astype(jnp.float32) * column_count
    )
    partial_value = selector[:, None] * power_mean[None, :]
    summed = lax.psum(partial_value, "elem")
    decibels = 10.0 * jnp.log10(summed + epsilon)
    return (formed.reshape(column_count, 2, beam_count), decibels)


def solution(mesh):
    n = mesh.shape["elem"]
    body = functools.partial(local_ring, n) if fits(mesh) else local
    return jax.shard_map(
        body,
        mesh=mesh,
        in_specs=(P(None, ("groups", "elem"), None), P(), P("groups"), P("groups"), P()),
        out_specs=(P("elem", None, "groups"), P(None, "groups")),
        check_vma=False,
    )
```

```python
import functools
import math

import jax
import jax.numpy as jnp
from jax import lax
from jax.experimental import pallas as pl
from jax.experimental.pallas import tpu as pltpu
from jax.sharding import PartitionSpec as P

epsilon = 1e-06
SIDE = 2
RING = 4
CHUNKS = 8


def band_of(band_len, position, unit_count):
    band_ends = jnp.cumsum(band_len)
    band_index = jnp.sum((band_ends <= position).astype(jnp.int32))
    selector = jnp.arange(band_len.shape[0], dtype=jnp.int32) == band_index
    band_size = jnp.sum(jnp.where(selector, band_len, 0))
    band_start = jnp.sum(jnp.where(selector, band_ends, 0)) - band_size
    frequency = (band_start.astype(jnp.float32) + 0.5 * band_size.astype(jnp.float32)) / float(
        unit_count
    )
    return (frequency, band_size, selector.astype(jnp.float32))


def sincos(turns):
    reduced = turns - jnp.floor(turns + 0.5)
    x = reduced * math.pi
    q = x * x
    sin_terms = [(-1.0) ** i / math.factorial(2 * i + 1) for i in range(7)]
    cos_terms = [(-1.0) ** i / math.factorial(2 * i) for i in range(8)]
    s = jnp.full_like(q, sin_terms[-1])
    for term in sin_terms[-2::-1]:
        s = s * q + term
    s = s * x
    c = jnp.full_like(q, cos_terms[-1])
    for term in cos_terms[-2::-1]:
        c = c * q + term
    return 2.0 * s * c, 1.0 - 2.0 * s * s


def split2(v):
    high = v.astype(jnp.bfloat16)
    return high, (v - high.astype(jnp.float32)).astype(jnp.bfloat16)


def split3(v):
    high = v.astype(jnp.bfloat16)
    rest = v - high.astype(jnp.float32)
    middle = rest.astype(jnp.bfloat16)
    return high, middle, (rest - middle.astype(jnp.float32)).astype(jnp.bfloat16)


def item_unit(i):
    return 3 - i + (i + RING) // (RING + 1) + i // (RING + 1)


def item_chunk(i):
    return CHUNKS - 2 + (i + RING) // (RING + 1) - i // (RING + 1)


def kernel(
    n, lens, x, delays, order, table, out, power, bands,
    bl, dl, od, tb, g1, dt, wh, wl, xa, xb, xz, pa, pb, ra, rb, ry, fin, tot,
    in_s, own_a, own_b, sa_s, sa_r, sb_s, sb_r, sy_s, sy_r, sz_s, sz_r,
    a_s, a_r, b_s, b_r, y2_s, y2_r, p_s, p_r,
):
    me = lax.axis_index("elem")
    core = me % SIDE
    y = (me // SIDE) % SIDE
    z = me // (SIDE * SIDE)
    upper = z // 2
    end = z + upper * (RING - 1 - 2 * z)
    unit_cols = x.shape[2] // n
    chunk = unit_cols // CHUNKS
    most = CHUNKS - 1
    beams = table.shape[1]
    scaling = float(delays.shape[1]) ** (-0.5)
    slots = (3, 2, 1 - end, end)
    early = (most - 1, most, most - end, most - 1 + end)

    def chip(u):
        return u + upper * (RING - 1 - 2 * u)

    def dev(zz, yy, cc):
        return (zz * SIDE + yy % SIDE) * SIDE + cc % SIDE

    ahead = dev(chip(end + 1), y, core)
    beside = dev(chip(1 - end), y, core)

    barrier = pltpu.get_barrier_semaphore()

    def greet(target):
        pl.semaphore_signal(barrier, inc=1, device_id={"elem": target},
                            device_id_type=pl.DeviceIdType.MESH)

    for r in (0, 1):
        greet(dev(z, y + 1, core + r))
        greet(dev(chip(1 - end), y, core + r))
    greet(dev(z, y, core + 1))

    @pl.when(end == 1)
    def _():
        greet(ahead)

    fetches = [
        pltpu.make_async_copy(lens, bl, in_s.at[0]),
        pltpu.make_async_copy(delays, dl, in_s.at[1]),
        pltpu.make_async_copy(order, od, in_s.at[2]),
        pltpu.make_async_copy(table, tb, in_s.at[3]),
    ]
    for fetch in fetches:
        fetch.start()
    pl.semaphore_wait(barrier, 5 + end)

    def remote(src, dst, send, recv, target):
        return pltpu.make_async_remote_copy(
            src_ref=src, dst_ref=dst, send_sem=send, recv_sem=recv,
            device_id={"elem": target}, device_id_type=pl.DeviceIdType.MESH)

    def cols(unit, start, size):
        return x.at[:, :, pl.ds(pl.multiple_of(unit * unit_cols + start, 128), size)]

    def part(k):
        return pl.ds(pl.multiple_of(k * chunk, 128), chunk)

    def y_copy(j, k, r):
        return remote(
            cols(dev(chip(slots[j]), y + 1, core + r), k * chunk, chunk),
            xa.at[2 + r, j, :, :, part(k)],
            sy_s.at[r, j, k], sy_r.at[r, j, k], dev(z, y + 1, core + r))

    def late(i, yy, cc):
        return cols(dev(chip(item_unit(i)), yy, cc), item_chunk(i) * chunk, chunk)

    def z_copy(i, yr, r):
        return remote(
            late(i, y + yr, core + r), xz.at[i, r, yr],
            sz_s.at[i, r, yr], sz_r.at[i, r, yr], dev(chip(1 - end), y, core + r))

    def b_peer(i, yr):
        return remote(late(i, y + yr, core + 1), xb.at[1, i, yr],
                      sb_s.at[i, yr], sb_r.at[i, yr], dev(z, y, core + 1))

    def b_own(i, yr):
        return pltpu.make_async_copy(late(i, y + yr, core), xb.at[0, i, yr], own_b.at[i, yr])

    def a_copy(j, k):
        to = j + 3 * end if j < 2 else 2
        return remote(pa.at[j, k], ra.at[to, k], a_s.at[j, k], a_r.at[to, k],
                      ahead if j < 2 else beside)

    def a_wait(to, k):
        remote(pa.at[0, k], ra.at[to, k], a_s.at[0, k], a_r.at[to, k], beside).wait_recv()

    def b_ahead(i, yr):
        return remote(pb.at[i, yr], rb.at[i, yr], b_s.at[i, yr], b_r.at[i, yr], ahead)

    def b_back(i, yr):
        return remote(pb.at[i, yr], rb.at[i - 1, yr], b_s.at[i - 1, yr], b_r.at[i - 1, yr],
                      beside)

    def last(i):
        return remote(pb.at[i, 1], ry.at[i - 3], y2_s.at[i - 3], y2_r.at[i - 3],
                      dev(z, y + 1, core))

    def every(low, high, step):
        def body(t, carry):
            step(t)
            return carry

        lax.fori_loop(low, high, body, 0)

    pairs = [(yr, r) for yr in (1, 0) for r in (0, 1)]

    def issue(low):
        def start(k):
            for r in (0, 1):
                y_copy(0, k, r).start()

        every(low, early[0], start)

        @pl.when(end == 0)
        def _():
            def start(t):
                for r in (0, 1):
                    z_copy(t // 2, 1 - t % 2, r).start()

            every(low, 8, start)

        for j in (1, 2, 3):
            def start(k, j=j):
                for r in (0, 1):
                    y_copy(j, k, r).start()

            every(0, early[j], start)

    first = 1
    for r in (0, 1)[:first]:
        y_copy(0, 0, r).start()

    @pl.when(end == 0)
    def _():
        for r in (0, 1)[:first]:
            z_copy(0, 1, r).start()

    def rest():
        for r in (0, 1)[first:]:
            y_copy(0, 0, r).start()

        @pl.when(end == 0)
        def _():
            for r in (0, 1)[first:]:
                z_copy(0, 1, r).start()

        issue(1)

    @pl.when(core == 0)
    def _():
        rest()

    ca, la = {}, {}

    def b_start(i):
        for yr in (1, 0):
            b_peer(i, yr).start()
            b_own(i, yr).start()

    for j in range(4):
        there = dev(chip(slots[j]), y, core + 1)
        here = dev(chip(slots[j]), y, core)
        ca[j] = remote(cols(there, 0, most * chunk), xa.at[1, j],
                       sa_s.at[j], sa_r.at[j], dev(z, y, core + 1))
        la[j] = pltpu.make_async_copy(cols(here, 0, most * chunk), xa.at[0, j], own_a.at[j])
        ca[j].start()
        la[j].start()
        if j == 0:
            every(4 - 4 * end, 6, b_start)

    for fetch in fetches:
        fetch.wait()

    def frequency(unit):
        total, value = 0, 0.0
        for b in range(lens.shape[0]):
            size = bl[b]
            inside = jnp.logical_and(unit >= total, unit < total + size)
            middle = (2 * total + size).astype(jnp.float32) * (0.5 / n)
            value = jnp.where(inside, middle, value)
            total = total + size
        return value

    band = lax.broadcasted_iota(jnp.int32, bands.shape[1:], 0)
    total = 0
    for b in range(lens.shape[0]):
        bands[0] = jnp.where(band == b, total, bands[0] if b else 0)
        bands[1] = jnp.where(band == b, bl[b], bands[1] if b else 0)
        total = total + bl[b]

    beam_hot = jnp.where(
        lax.broadcasted_iota(jnp.int32, (delays.shape[0], beams), 0) == tb[...], 1.0, 0.0
    ).T.astype(jnp.bfloat16)
    step = 512 if delays.shape[1] % 512 == 0 else delays.shape[1]

    def pick_beams(i):
        span = pl.ds(pl.multiple_of(i * step, step), step)
        parts = split3(dl[:, span])
        rows = [jnp.dot(beam_hot, piece, preferred_element_type=jnp.float32) for piece in parts]
        for m, piece in enumerate(rows):
            g1[m * beams:(m + 1) * beams, span] = piece.astype(jnp.bfloat16)

    every(0, delays.shape[1] // step, pick_beams)

    def pick_elems(s):
        r, g = s % 2, s // 2
        u = end + (g // 2) * (1 - 2 * end)
        q = dev(chip(u), y + g % 2, core + r)
        row = od[q]
        hot = jnp.where(
            lax.broadcasted_iota(jnp.int32, (delays.shape[1], row.shape[1]), 0) == row, 1.0, 0.0
        ).astype(jnp.bfloat16)
        got = jnp.dot(g1[...], hot, preferred_element_type=jnp.float32)
        dt[s] = got[:beams] + got[beams:2 * beams] + got[2 * beams:]

    every(0, 2, pick_elems)

    @pl.when(core == 1)
    def _():
        rest()

    every(2, 6, pick_elems)
    wide = 2 * x.shape[1]

    def weigh(f, sources):
        for i, s in enumerate(sources):
            sine, cosine = sincos(f * dt[s])
            ch, cl = split2(cosine * scaling)
            sh, sl = split2(sine * scaling)
            span = slice(i * wide, (i + 1) * wide)
            wh[:beams, span] = jnp.concatenate([ch, sh], axis=1)
            wh[beams:, span] = jnp.concatenate([-sh, ch], axis=1)
            wl[:beams, span] = jnp.concatenate([cl, sl], axis=1)
            wl[beams:, span] = jnp.concatenate([-sl, cl], axis=1)

    def form(pieces):
        rows = jnp.concatenate([piece.reshape(wide, chunk) for piece in pieces], axis=0)
        xh, xl = split2(rows)
        span = slice(0, wide * len(pieces))
        dot = functools.partial(jnp.dot, preferred_element_type=jnp.float32)
        high = wh[:, span]
        return dot(high, xh) + (dot(high, xl) + dot(wl[:, span], xh))

    def a_slot(j, then, pause=None):
        weigh(frequency(dev(chip(slots[j]), y, core)), (0, 1, 2, 3))
        la[j].wait()
        ca[j].wait_recv()

        def one(k):
            for r in (0, 1):
                y_copy(j, k, r).wait_recv()
            pa[j, k] = form([xa[s, j, :, :, part(k)] for s in range(4)])
            then(k)

        if pause is None:
            every(0, early[j], one)
        else:
            every(0, early[j] - 1, one)
            pause()
            one(early[j] - 1)

    def join(j, to, k):
        a_wait(to, k)
        pa[j, k] += ra[to, k]

    def after0(k):
        @pl.when(end == 0)
        def _():
            a_copy(0, k).start()

    def join0(k):
        join(0, 0, k)
        a_copy(0, k).start()

    def join1(k):
        join(1, 1, k)
        a_copy(1, k).start()

    def after1(k):
        @pl.when(end == 0)
        def _():
            a_copy(1, k).start()

        @pl.when(jnp.logical_and(end == 1, k < early[0]))
        def _():
            join0(k)

    def after2(k):
        @pl.when(end == 1)
        def _():
            join(2, 3, k)

        a_copy(2, k).start()

        @pl.when(end == 1)
        def _():
            join1(k)

    def put(got, start):
        rows = pl.ds(pl.multiple_of(start, 128), chunk)
        out[rows, 0, :] = got[:, :beams]
        out[rows, 1, :] = got[:, beams:]

    def emit(got, start):
        put(got, start)
        tot[...] += jnp.sum(got * got, axis=0, keepdims=True)

    def after3(k):
        @pl.when(end == 1)
        def _():
            join(3, 4, k)

        a_wait(2, k)

        @pl.when(k < most - 1)
        def _():
            emit((pa[3, k] + ra[2, k]).T, k * chunk)

    tot[...] = jnp.zeros_like(tot)

    def b_landed(i, yr):
        b_own(i, yr).wait()
        b_peer(i, yr).wait_recv()

    def b_joint(i, yr):
        for r in (0, 1):
            z_copy(i, yr, r).wait_recv()
        b_landed(i, yr)
        weigh(frequency(dev(chip(item_unit(i)), y + yr, core)), (0, 1, 4, 5))
        pb[i, yr] = form([xb[0, i, yr], xb[1, i, yr], xz[i, 0, yr], xz[i, 1, yr]])

    @pl.when(end == 1)
    def _():
        def b_first(t):
            i, yr = t // 2, 1 - t % 2
            b_joint(i, yr)
            b_ahead(i, yr).start()

        every(0, 6, b_first)

    a_slot(0, after0)

    def b_end(t):
        i, yr = 4 + t % 2, 1 - t // 2
        b_landed(i, yr)
        weigh(frequency(dev(chip(0), y + yr, core)), (0, 1))
        pb[i, yr] = form([xb[0, i, yr], xb[1, i, yr]])

    every(0, 4, b_end)
    a_slot(1, after1)

    @pl.when(end == 1)
    def _():
        for i in range(2):
            for yr in (1, 0):
                b_ahead(i, yr).wait_recv()
                pb[5 - i, yr] += rb[i, yr]
                b_back(5 - i, yr).start()

        def b_home(t):
            yr = 1 - t
            b_joint(3, yr)
            b_ahead(2, yr).wait_recv()
            pb[3, yr] += rb[2, yr]

        every(0, 2, b_home)

    a_slot(2, after2)

    @pl.when(end == 1)
    def _():
        join1(most - 1)
        last(3).start()

    @pl.when(end == 0)
    def _():
        for i in (4, 5):
            for yr in (1, 0):
                b_back(i, yr).wait_recv()
                pb[i, yr] += rb[i - 1, yr]
            last(i).start()

    def finish(i):
        last(i).wait_recv()
        emit((pb[i, 0] + ry[i - 3]).T, item_chunk(i) * chunk)

    a_slot(3, after3, lambda: every(3, 3 + end, finish))

    @pl.when(end == 0)
    def _():
        finish(4)
        last(5).wait_recv()
        fin[...] = pb[5, 0] + ry[2]

    @pl.when(end == 1)
    def _():
        fin[...] = pa[3, most - 1] + ra[2, most - 1]

    squares = fin[...] * fin[...]
    late_row = jnp.sum((squares[:beams] + squares[beams:]).T, axis=0, keepdims=True)
    power[me] = tot[:, :beams] + tot[:, beams:] + late_row

    def p_copy(target):
        return remote(power.at[me], power.at[me], p_s, p_r, target)

    def p_far(t):
        p_copy(dev(chip(3 - t // (SIDE * SIDE)), y + 1 + t // SIDE, core + t)).start()

    others = 3 - end
    every(0, others * SIDE * SIDE, p_far)

    @pl.when(end == 1)
    def _():
        for t in range(SIDE * SIDE):
            p_copy(dev(chip(0), y + 1 + t // SIDE, core + t)).start()

    for t in range(SIDE * SIDE - 1):
        p_copy(dev(z, y + 1 + t // SIDE, core + t + t // SIDE)).start()

    put(fin[...].T, (most - 1) * chunk)

    def last_sent(i):
        last(i).wait_send()

    every(4 - end, 6 - 2 * end, last_sent)

    def b_sent(i):
        for yr in (1, 0):
            b_peer(i, yr).wait_send()

    every(4 - 4 * end, 6, b_sent)
    for j in range(4):
        ca[j].wait_send()

        def drain(k, j=j):
            for r in (0, 1):
                y_copy(j, k, r).wait_send()
            if j < 3:
                a_copy(j, k).wait_send()

        every(0, early[j], drain)

    @pl.when(end == 0)
    def _():
        def z_sent(i):
            for yr, r in pairs:
                z_copy(i, yr, r).wait_send()

        every(0, 4, z_sent)

    @pl.when(end == 1)
    def _():
        for yr in (1, 0):
            for i in range(3):
                b_ahead(i, yr).wait_send()
            for i in (4, 5):
                b_back(i, yr).wait_send()

    rest = power.at[pl.ds(0, n - 1)]
    remote(rest, rest, p_s, p_r, beside).wait()


def conclude(n, formed, power, bands, beams, decibels, level, sems):
    pieces = sems.shape[0] - 1
    rows = formed.shape[0] // pieces
    copies = []
    for i in range(pieces):
        span = pl.ds(i * rows, rows)
        copies.append(pltpu.make_async_copy(formed.at[span], beams.at[span], sems.at[i]))
        copies[-1].start()
    low, size = bands[0], bands[1]
    high = low + size
    summed = jnp.zeros(level.shape, jnp.float32)
    for u in range(n):
        inside = jnp.logical_and(low <= u, u < high)
        summed = summed + jnp.where(inside, power[u], 0.0)
    mean = summed / (size.astype(jnp.float32) * formed.shape[0])
    level[...] = (10.0 / math.log(10.0)) * jnp.log(mean + epsilon)
    copies.append(pltpu.make_async_copy(level, decibels, sems.at[pieces]))
    copies[-1].start()
    for copy in copies:
        copy.wait()


def local_ring(n, snapshots, delays, element_order, beam_table, band_len):
    local_elems = snapshots.shape[1]
    unit_cols = snapshots.shape[2] // n
    beams = beam_table.shape[0]
    most, chunk = CHUNKS - 1, unit_cols // CHUNKS
    block = (2 * beams, chunk)
    f32, sem = jnp.float32, pltpu.SemaphoreType.DMA
    raw = (2, local_elems)
    vmem, hbm = (pl.BlockSpec(memory_space=m) for m in (pltpu.VMEM, pl.ANY))
    band_shape = (band_len.shape[0], beams)
    formed, power, bands = pl.pallas_call(
        functools.partial(kernel, n),
        out_shape=(
            pltpu.VMEM((unit_cols, 2, beams), f32),
            pltpu.VMEM((n, 1, beams), f32),
            pltpu.VMEM((2,) + band_shape, jnp.int32),
        ),
        in_specs=[hbm] * 5,
        out_specs=(vmem, vmem, vmem),
        scratch_shapes=[
            pltpu.SMEM(band_len.shape, jnp.int32),
            pltpu.VMEM(delays.shape, f32),
            pltpu.VMEM((n, 1, local_elems), jnp.int32),
            pltpu.VMEM((1, beams), jnp.int32),
            pltpu.VMEM((3 * beams, delays.shape[1]), jnp.bfloat16),
            pltpu.VMEM((6, beams, local_elems), f32),
            pltpu.VMEM((2 * beams, 8 * local_elems), jnp.bfloat16),
            pltpu.VMEM((2 * beams, 8 * local_elems), jnp.bfloat16),
            pltpu.VMEM((4, 4) + raw + (most * chunk,), f32),
            pltpu.VMEM((2, 6, 2) + raw + (chunk,), f32),
            pltpu.VMEM((4, 2, 2) + raw + (chunk,), f32),
            pltpu.VMEM((4, most) + block, f32),
            pltpu.VMEM((6, 2) + block, f32),
            pltpu.VMEM((5, most) + block, f32),
            pltpu.VMEM((5, 2) + block, f32),
            pltpu.VMEM((3,) + block, f32),
            pltpu.VMEM(block, f32),
            pltpu.VMEM((1, 2 * beams), f32),
            sem((4,)), sem((4,)), sem((6, 2)),
            sem((4,)), sem((4,)), sem((6, 2)), sem((6, 2)),
            sem((2, 4, most)), sem((2, 4, most)), sem((4, 2, 2)), sem((4, 2, 2)),
            sem((3, most)), sem((5, most)), sem((5, 2)), sem((5, 2)),
            sem((3,)), sem((3,)),
            sem, sem,
        ],
        compiler_params=pltpu.CompilerParams(
            collective_id=0, has_side_effects=True, vmem_limit_bytes=54 * 1024 * 1024
        ),
    )(
        band_len, snapshots, delays,
        element_order.reshape(n, 1, local_elems), beam_table.reshape(1, beams),
    )
    parts = [pltpu.with_memory_space_constraint(v, pltpu.VMEM) for v in (formed, power, bands)]
    return pl.pallas_call(
        functools.partial(conclude, n),
        out_shape=(
            jax.ShapeDtypeStruct((unit_cols, 2, beams), f32),
            jax.ShapeDtypeStruct(band_shape, f32),
        ),
        in_specs=[vmem] * 3,
        out_specs=(hbm, hbm),
        scratch_shapes=[pltpu.VMEM(band_shape, f32), sem((9,))],
    )(*parts)


def fits(mesh):
    return mesh.shape["elem"] == SIDE * SIDE * RING


def steering(delays, element_order, beam_table, frequency):
    delay_rows = jnp.take(delays, beam_table, axis=0)
    delay_rows = jnp.take(delay_rows, element_order, axis=1)
    phases = 2.0 * math.pi * frequency * delay_rows
    scaling = float(delays.shape[1]) ** (-0.5)
    cosines = jnp.cos(phases) * scaling
    sines = -jnp.sin(phases) * scaling
    upper_rows = jnp.concatenate([cosines.T, sines.T], axis=1)
    lower_rows = jnp.concatenate([-sines.T, cosines.T], axis=1)
    return jnp.concatenate([upper_rows, lower_rows], axis=0)


def project(arrived, weights):
    columns = arrived.shape[2]
    stacked = arrived.reshape(2 * arrived.shape[1], columns)
    return lax.dot_general(
        stacked,
        weights,
        (((0,), (0,)), ((), ())),
        precision=lax.Precision.HIGHEST,
        preferred_element_type=jnp.float32,
    )


def local(snapshots, delays, element_order, beam_table, band_len):
    unit_count = lax.axis_size("elem")
    position = lax.axis_index("elem")
    frequency, band_size, selector = band_of(band_len, position, unit_count)
    weights = steering(delays, element_order, beam_table, frequency)
    beam_count = beam_table.shape[0]
    local_elems = snapshots.shape[1]
    unit_cols = snapshots.shape[2] // unit_count
    divided = snapshots.reshape(2, local_elems, unit_count, unit_cols)
    pieces = lax.all_to_all(divided, "elem", split_axis=2, concat_axis=1, tiled=True)
    formed = project(pieces.reshape(2, pieces.shape[1], pieces.shape[3]), weights)
    column_count = formed.shape[0]
    squares = jnp.sum(formed * formed, axis=0)
    power_mean = (squares[:beam_count] + squares[beam_count:]) / (
        band_size.astype(jnp.float32) * column_count
    )
    partial_value = selector[:, None] * power_mean[None, :]
    summed = lax.psum(partial_value, "elem")
    decibels = 10.0 * jnp.log10(summed + epsilon)
    return (formed.reshape(column_count, 2, beam_count), decibels)


def solution(mesh):
    n = mesh.shape["elem"]
    body = functools.partial(local_ring, n) if fits(mesh) else local
    return jax.shard_map(
        body,
        mesh=mesh,
        in_specs=(P(None, ("groups", "elem"), None), P(), P("groups"), P("groups"), P()),
        out_specs=(P("elem", None, "groups"), P(None, "groups")),
        check_vma=False,
    )
```

```python
import functools
import math

import jax
import jax.numpy as jnp
from jax import lax
from jax.experimental import pallas as pl
from jax.experimental.pallas import tpu as pltpu
from jax.sharding import PartitionSpec as P

epsilon = 1e-06
SIDE = 2
RING = 4
CHUNKS = 8


def band_of(band_len, position, unit_count):
    band_ends = jnp.cumsum(band_len)
    band_index = jnp.sum((band_ends <= position).astype(jnp.int32))
    selector = jnp.arange(band_len.shape[0], dtype=jnp.int32) == band_index
    band_size = jnp.sum(jnp.where(selector, band_len, 0))
    band_start = jnp.sum(jnp.where(selector, band_ends, 0)) - band_size
    frequency = (band_start.astype(jnp.float32) + 0.5 * band_size.astype(jnp.float32)) / float(
        unit_count
    )
    return (frequency, band_size, selector.astype(jnp.float32))


def sincos(turns):
    reduced = turns - jnp.floor(turns + 0.5)
    x = reduced * math.pi
    q = x * x
    sin_terms = [(-1.0) ** i / math.factorial(2 * i + 1) for i in range(7)]
    cos_terms = [(-1.0) ** i / math.factorial(2 * i) for i in range(8)]
    s = jnp.full_like(q, sin_terms[-1])
    for term in sin_terms[-2::-1]:
        s = s * q + term
    s = s * x
    c = jnp.full_like(q, cos_terms[-1])
    for term in cos_terms[-2::-1]:
        c = c * q + term
    return 2.0 * s * c, 1.0 - 2.0 * s * s


def split2(v):
    high = v.astype(jnp.bfloat16)
    return high, (v - high.astype(jnp.float32)).astype(jnp.bfloat16)


def split3(v):
    high = v.astype(jnp.bfloat16)
    rest = v - high.astype(jnp.float32)
    middle = rest.astype(jnp.bfloat16)
    return high, middle, (rest - middle.astype(jnp.float32)).astype(jnp.bfloat16)


def item_unit(i):
    return 3 - i + (i + RING) // (RING + 1) + i // (RING + 1)


def item_chunk(i):
    return CHUNKS - 2 + (i + RING) // (RING + 1) - i // (RING + 1)


def kernel(
    n, lens, x, delays, order, table, out, power, bands,
    bl, dl, od, tb, g1, dt, wh, wl, xa, xb, xz, pa, pb, ra, rb, ry, fin, tot,
    in_s, own_a, own_b, sa_s, sa_r, sb_s, sb_r, sy_s, sy_r, sz_s, sz_r,
    a_s, a_r, b_s, b_r, y2_s, y2_r, p_s, p_r,
):
    me = lax.axis_index("elem")
    core = me % SIDE
    y = (me // SIDE) % SIDE
    z = me // (SIDE * SIDE)
    upper = z // 2
    end = z + upper * (RING - 1 - 2 * z)
    unit_cols = x.shape[2] // n
    chunk = unit_cols // CHUNKS
    most = CHUNKS - 1
    beams = table.shape[1]
    scaling = float(delays.shape[1]) ** (-0.5)
    slots = (3, 2, 1 - end, end)
    early = (most - 1, most, most - end, most - 1 + end)

    def chip(u):
        return u + upper * (RING - 1 - 2 * u)

    def dev(zz, yy, cc):
        return (zz * SIDE + yy % SIDE) * SIDE + cc % SIDE

    ahead = dev(chip(end + 1), y, core)
    beside = dev(chip(1 - end), y, core)

    barrier = pltpu.get_barrier_semaphore()

    def greet(target):
        pl.semaphore_signal(barrier, inc=1, device_id={"elem": target},
                            device_id_type=pl.DeviceIdType.MESH)

    for r in (0, 1):
        greet(dev(z, y + 1, core + r))
        greet(dev(chip(1 - end), y, core + r))
    greet(dev(z, y, core + 1))

    @pl.when(end == 1)
    def _():
        greet(ahead)

    fetches = [
        pltpu.make_async_copy(lens, bl, in_s.at[0]),
        pltpu.make_async_copy(delays, dl, in_s.at[1]),
        pltpu.make_async_copy(order, od, in_s.at[2]),
        pltpu.make_async_copy(table, tb, in_s.at[3]),
    ]
    for fetch in fetches:
        fetch.start()
    pl.semaphore_wait(barrier, 5 + end)

    def remote(src, dst, send, recv, target):
        return pltpu.make_async_remote_copy(
            src_ref=src, dst_ref=dst, send_sem=send, recv_sem=recv,
            device_id={"elem": target}, device_id_type=pl.DeviceIdType.MESH)

    def cols(unit, start, size):
        return x.at[:, :, pl.ds(pl.multiple_of(unit * unit_cols + start, 128), size)]

    def part(k):
        return pl.ds(pl.multiple_of(k * chunk, 128), chunk)

    def y_copy(j, k, r):
        return remote(
            cols(dev(chip(slots[j]), y + 1, core + r), k * chunk, chunk),
            xa.at[2 + r, j, :, :, part(k)],
            sy_s.at[r, j, k], sy_r.at[r, j, k], dev(z, y + 1, core + r))

    def late(i, yy, cc):
        return cols(dev(chip(item_unit(i)), yy, cc), item_chunk(i) * chunk, chunk)

    def z_copy(i, yr, r):
        return remote(
            late(i, y + yr, core + r), xz.at[i, r, yr],
            sz_s.at[i, r, yr], sz_r.at[i, r, yr], dev(chip(1 - end), y, core + r))

    def b_peer(i, yr):
        return remote(late(i, y + yr, core + 1), xb.at[1, i, yr],
                      sb_s.at[i, yr], sb_r.at[i, yr], dev(z, y, core + 1))

    def b_own(i, yr):
        return pltpu.make_async_copy(late(i, y + yr, core), xb.at[0, i, yr], own_b.at[i, yr])

    def a_copy(j, k):
        to = j + 3 * end if j < 2 else 2
        return remote(pa.at[j, k], ra.at[to, k], a_s.at[j, k], a_r.at[to, k],
                      ahead if j < 2 else beside)

    def a_wait(to, k):
        remote(pa.at[0, k], ra.at[to, k], a_s.at[0, k], a_r.at[to, k], beside).wait_recv()

    def b_ahead(i, yr):
        return remote(pb.at[i, yr], rb.at[i, yr], b_s.at[i, yr], b_r.at[i, yr], ahead)

    def b_back(i, yr):
        return remote(pb.at[i, yr], rb.at[i - 1, yr], b_s.at[i - 1, yr], b_r.at[i - 1, yr],
                      beside)

    def last(i):
        return remote(pb.at[i, 1], ry.at[i - 3], y2_s.at[i - 3], y2_r.at[i - 3],
                      dev(z, y + 1, core))

    def every(low, high, step):
        def body(t, carry):
            step(t)
            return carry

        lax.fori_loop(low, high, body, 0)

    pairs = [(yr, r) for yr in (1, 0) for r in (0, 1)]

    def issue():
        def start(k):
            for r in (0, 1):
                y_copy(0, k, r).start()

        every(1, early[0], start)

        @pl.when(end == 0)
        def _():
            def start(t):
                for r in (0, 1):
                    z_copy(t // 2, 1 - t % 2, r).start()

            every(1, 8, start)

        for j in (1, 2, 3):
            def start(k, j=j):
                for r in (0, 1):
                    y_copy(j, k, r).start()

            every(0, early[j], start)

    y_copy(0, 0, 0).start()

    @pl.when(end == 0)
    def _():
        z_copy(0, 1, 0).start()

    def rest():
        y_copy(0, 0, 1).start()

        @pl.when(end == 0)
        def _():
            z_copy(0, 1, 1).start()

        issue()

    @pl.when(core == 0)
    def _():
        rest()

    ca, la = {}, {}

    def b_start(i):
        for yr in (1, 0):
            b_peer(i, yr).start()
            b_own(i, yr).start()

    for j in range(4):
        there = dev(chip(slots[j]), y, core + 1)
        here = dev(chip(slots[j]), y, core)
        ca[j] = remote(cols(there, 0, most * chunk), xa.at[1, j],
                       sa_s.at[j], sa_r.at[j], dev(z, y, core + 1))
        la[j] = pltpu.make_async_copy(cols(here, 0, most * chunk), xa.at[0, j], own_a.at[j])
        ca[j].start()
        la[j].start()
        if j == 0:
            every(4 - 4 * end, 6, b_start)

    for fetch in fetches:
        fetch.wait()

    def frequency(unit):
        total, value = 0, 0.0
        for b in range(lens.shape[0]):
            size = bl[b]
            inside = jnp.logical_and(unit >= total, unit < total + size)
            middle = (2 * total + size).astype(jnp.float32) * (0.5 / n)
            value = jnp.where(inside, middle, value)
            total = total + size
        return value

    band = lax.broadcasted_iota(jnp.int32, bands.shape[1:], 0)
    total = 0
    for b in range(lens.shape[0]):
        bands[0] = jnp.where(band == b, total, bands[0] if b else 0)
        bands[1] = jnp.where(band == b, bl[b], bands[1] if b else 0)
        total = total + bl[b]

    beam_hot = jnp.where(
        lax.broadcasted_iota(jnp.int32, (delays.shape[0], beams), 0) == tb[...], 1.0, 0.0
    ).T.astype(jnp.bfloat16)
    step = 512 if delays.shape[1] % 512 == 0 else delays.shape[1]

    def pick_beams(i):
        span = pl.ds(pl.multiple_of(i * step, step), step)
        parts = split3(dl[:, span])
        rows = [jnp.dot(beam_hot, piece, preferred_element_type=jnp.float32) for piece in parts]
        for m, piece in enumerate(rows):
            g1[m * beams:(m + 1) * beams, span] = piece.astype(jnp.bfloat16)

    every(0, delays.shape[1] // step, pick_beams)

    def pick_elems(s):
        r, g = s % 2, s // 2
        u = end + (g // 2) * (1 - 2 * end)
        q = dev(chip(u), y + g % 2, core + r)
        row = od[q]
        hot = jnp.where(
            lax.broadcasted_iota(jnp.int32, (delays.shape[1], row.shape[1]), 0) == row, 1.0, 0.0
        ).astype(jnp.bfloat16)
        got = jnp.dot(g1[...], hot, preferred_element_type=jnp.float32)
        dt[s] = got[:beams] + got[beams:2 * beams] + got[2 * beams:]

    every(0, 1, pick_elems)

    @pl.when(core == 1)
    def _():
        rest()

    every(1, 6, pick_elems)
    wide = 2 * x.shape[1]

    def weigh(f, sources):
        for i, s in enumerate(sources):
            sine, cosine = sincos(f * dt[s])
            ch, cl = split2(cosine * scaling)
            sh, sl = split2(sine * scaling)
            span = slice(i * wide, (i + 1) * wide)
            wh[:beams, span] = jnp.concatenate([ch, sh], axis=1)
            wh[beams:, span] = jnp.concatenate([-sh, ch], axis=1)
            wl[:beams, span] = jnp.concatenate([cl, sl], axis=1)
            wl[beams:, span] = jnp.concatenate([-sl, cl], axis=1)

    def form(pieces):
        rows = jnp.concatenate([piece.reshape(wide, chunk) for piece in pieces], axis=0)
        xh, xl = split2(rows)
        span = slice(0, wide * len(pieces))
        dot = functools.partial(jnp.dot, preferred_element_type=jnp.float32)
        high = wh[:, span]
        return dot(high, xh) + (dot(high, xl) + dot(wl[:, span], xh))

    def a_slot(j, then, pause=None):
        weigh(frequency(dev(chip(slots[j]), y, core)), (0, 1, 2, 3))
        la[j].wait()
        ca[j].wait_recv()

        def one(k):
            for r in (0, 1):
                y_copy(j, k, r).wait_recv()
            pa[j, k] = form([xa[s, j, :, :, part(k)] for s in range(4)])
            then(k)

        if pause is None:
            every(0, early[j], one)
        else:
            every(0, early[j] - 1, one)
            pause()
            one(early[j] - 1)

    def join(j, to, k):
        a_wait(to, k)
        pa[j, k] += ra[to, k]

    def after0(k):
        @pl.when(end == 0)
        def _():
            a_copy(0, k).start()

    def join0(k):
        join(0, 0, k)
        a_copy(0, k).start()

    def join1(k):
        join(1, 1, k)
        a_copy(1, k).start()

    def after1(k):
        @pl.when(end == 0)
        def _():
            a_copy(1, k).start()

        @pl.when(jnp.logical_and(end == 1, k < early[0]))
        def _():
            join0(k)

    def after2(k):
        @pl.when(end == 1)
        def _():
            join(2, 3, k)

        a_copy(2, k).start()

        @pl.when(end == 1)
        def _():
            join1(k)

    def put(got, start):
        rows = pl.ds(pl.multiple_of(start, 128), chunk)
        out[rows, 0, :] = got[:, :beams]
        out[rows, 1, :] = got[:, beams:]

    def emit(got, start):
        put(got, start)
        tot[...] += jnp.sum(got * got, axis=0, keepdims=True)

    def after3(k):
        @pl.when(end == 1)
        def _():
            join(3, 4, k)

        a_wait(2, k)

        @pl.when(k < most - 1)
        def _():
            emit((pa[3, k] + ra[2, k]).T, k * chunk)

    tot[...] = jnp.zeros_like(tot)

    def b_landed(i, yr):
        b_own(i, yr).wait()
        b_peer(i, yr).wait_recv()

    def b_joint(i, yr):
        for r in (0, 1):
            z_copy(i, yr, r).wait_recv()
        b_landed(i, yr)
        weigh(frequency(dev(chip(item_unit(i)), y + yr, core)), (0, 1, 4, 5))
        pb[i, yr] = form([xb[0, i, yr], xb[1, i, yr], xz[i, 0, yr], xz[i, 1, yr]])

    @pl.when(end == 1)
    def _():
        def b_first(t):
            i, yr = t // 2, 1 - t % 2
            b_joint(i, yr)
            b_ahead(i, yr).start()

        every(0, 6, b_first)

    a_slot(0, after0)

    def b_end(t):
        i, yr = 4 + t % 2, 1 - t // 2
        b_landed(i, yr)
        weigh(frequency(dev(chip(0), y + yr, core)), (0, 1))
        pb[i, yr] = form([xb[0, i, yr], xb[1, i, yr]])

    every(0, 4, b_end)
    a_slot(1, after1)

    @pl.when(end == 1)
    def _():
        for i in range(2):
            for yr in (1, 0):
                b_ahead(i, yr).wait_recv()
                pb[5 - i, yr] += rb[i, yr]
                b_back(5 - i, yr).start()

        def b_home(t):
            yr = 1 - t
            b_joint(3, yr)
            b_ahead(2, yr).wait_recv()
            pb[3, yr] += rb[2, yr]

        every(0, 2, b_home)

    a_slot(2, after2)

    @pl.when(end == 1)
    def _():
        join1(most - 1)
        last(3).start()

    @pl.when(end == 0)
    def _():
        for i in (4, 5):
            for yr in (1, 0):
                b_back(i, yr).wait_recv()
                pb[i, yr] += rb[i - 1, yr]
            last(i).start()

    def finish(i):
        last(i).wait_recv()
        emit((pb[i, 0] + ry[i - 3]).T, item_chunk(i) * chunk)

    a_slot(3, after3, lambda: every(3, 3 + end, finish))

    @pl.when(end == 0)
    def _():
        finish(4)
        last(5).wait_recv()
        fin[...] = pb[5, 0] + ry[2]

    @pl.when(end == 1)
    def _():
        fin[...] = pa[3, most - 1] + ra[2, most - 1]

    squares = fin[...] * fin[...]
    late_row = jnp.sum((squares[:beams] + squares[beams:]).T, axis=0, keepdims=True)
    power[me] = tot[:, :beams] + tot[:, beams:] + late_row

    def p_copy(target):
        return remote(power.at[me], power.at[me], p_s, p_r, target)

    def p_far(t):
        p_copy(dev(chip(3 - t // (SIDE * SIDE)), y + 1 + t // SIDE, core + t)).start()

    others = 3 - end
    every(0, others * SIDE * SIDE, p_far)

    @pl.when(end == 1)
    def _():
        for t in range(SIDE * SIDE):
            p_copy(dev(chip(0), y + 1 + t // SIDE, core + t)).start()

    for t in range(SIDE * SIDE - 1):
        p_copy(dev(z, y + 1 + t // SIDE, core + t + t // SIDE)).start()

    put(fin[...].T, (most - 1) * chunk)

    def last_sent(i):
        last(i).wait_send()

    every(4 - end, 6 - 2 * end, last_sent)

    def b_sent(i):
        for yr in (1, 0):
            b_peer(i, yr).wait_send()

    every(4 - 4 * end, 6, b_sent)
    for j in range(4):
        ca[j].wait_send()

        def drain(k, j=j):
            for r in (0, 1):
                y_copy(j, k, r).wait_send()
            if j < 3:
                a_copy(j, k).wait_send()

        every(0, early[j], drain)

    @pl.when(end == 0)
    def _():
        def z_sent(i):
            for yr, r in pairs:
                z_copy(i, yr, r).wait_send()

        every(0, 4, z_sent)

    @pl.when(end == 1)
    def _():
        for yr in (1, 0):
            for i in range(3):
                b_ahead(i, yr).wait_send()
            for i in (4, 5):
                b_back(i, yr).wait_send()

    rest = power.at[pl.ds(0, n - 1)]
    remote(rest, rest, p_s, p_r, beside).wait()


def conclude(n, formed, power, bands, beams, decibels, level, sems):
    pieces = sems.shape[0] - 1
    rows = formed.shape[0] // pieces
    copies = []
    for i in range(pieces):
        span = pl.ds(i * rows, rows)
        copies.append(pltpu.make_async_copy(formed.at[span], beams.at[span], sems.at[i]))
        copies[-1].start()
    low, size = bands[0], bands[1]
    high = low + size
    summed = jnp.zeros(level.shape, jnp.float32)
    for u in range(n):
        inside = jnp.logical_and(low <= u, u < high)
        summed = summed + jnp.where(inside, power[u], 0.0)
    mean = summed / (size.astype(jnp.float32) * formed.shape[0])
    level[...] = (10.0 / math.log(10.0)) * jnp.log(mean + epsilon)
    copies.append(pltpu.make_async_copy(level, decibels, sems.at[pieces]))
    copies[-1].start()
    for copy in copies:
        copy.wait()


def local_ring(n, snapshots, delays, element_order, beam_table, band_len):
    local_elems = snapshots.shape[1]
    unit_cols = snapshots.shape[2] // n
    beams = beam_table.shape[0]
    most, chunk = CHUNKS - 1, unit_cols // CHUNKS
    block = (2 * beams, chunk)
    f32, sem = jnp.float32, pltpu.SemaphoreType.DMA
    raw = (2, local_elems)
    vmem, hbm = (pl.BlockSpec(memory_space=m) for m in (pltpu.VMEM, pl.ANY))
    band_shape = (band_len.shape[0], beams)
    formed, power, bands = pl.pallas_call(
        functools.partial(kernel, n),
        out_shape=(
            pltpu.VMEM((unit_cols, 2, beams), f32),
            pltpu.VMEM((n, 1, beams), f32),
            pltpu.VMEM((2,) + band_shape, jnp.int32),
        ),
        in_specs=[hbm] * 5,
        out_specs=(vmem, vmem, vmem),
        scratch_shapes=[
            pltpu.SMEM(band_len.shape, jnp.int32),
            pltpu.VMEM(delays.shape, f32),
            pltpu.VMEM((n, 1, local_elems), jnp.int32),
            pltpu.VMEM((1, beams), jnp.int32),
            pltpu.VMEM((3 * beams, delays.shape[1]), jnp.bfloat16),
            pltpu.VMEM((6, beams, local_elems), f32),
            pltpu.VMEM((2 * beams, 8 * local_elems), jnp.bfloat16),
            pltpu.VMEM((2 * beams, 8 * local_elems), jnp.bfloat16),
            pltpu.VMEM((4, 4) + raw + (most * chunk,), f32),
            pltpu.VMEM((2, 6, 2) + raw + (chunk,), f32),
            pltpu.VMEM((4, 2, 2) + raw + (chunk,), f32),
            pltpu.VMEM((4, most) + block, f32),
            pltpu.VMEM((6, 2) + block, f32),
            pltpu.VMEM((5, most) + block, f32),
            pltpu.VMEM((5, 2) + block, f32),
            pltpu.VMEM((3,) + block, f32),
            pltpu.VMEM(block, f32),
            pltpu.VMEM((1, 2 * beams), f32),
            sem((4,)), sem((4,)), sem((6, 2)),
            sem((4,)), sem((4,)), sem((6, 2)), sem((6, 2)),
            sem((2, 4, most)), sem((2, 4, most)), sem((4, 2, 2)), sem((4, 2, 2)),
            sem((3, most)), sem((5, most)), sem((5, 2)), sem((5, 2)),
            sem((3,)), sem((3,)),
            sem, sem,
        ],
        compiler_params=pltpu.CompilerParams(
            collective_id=0, has_side_effects=True, vmem_limit_bytes=54 * 1024 * 1024
        ),
    )(
        band_len, snapshots, delays,
        element_order.reshape(n, 1, local_elems), beam_table.reshape(1, beams),
    )
    parts = [pltpu.with_memory_space_constraint(v, pltpu.VMEM) for v in (formed, power, bands)]
    return pl.pallas_call(
        functools.partial(conclude, n),
        out_shape=(
            jax.ShapeDtypeStruct((unit_cols, 2, beams), f32),
            jax.ShapeDtypeStruct(band_shape, f32),
        ),
        in_specs=[vmem] * 3,
        out_specs=(hbm, hbm),
        scratch_shapes=[pltpu.VMEM(band_shape, f32), sem((9,))],
    )(*parts)


def fits(mesh):
    return mesh.shape["elem"] == SIDE * SIDE * RING


def steering(delays, element_order, beam_table, frequency):
    delay_rows = jnp.take(delays, beam_table, axis=0)
    delay_rows = jnp.take(delay_rows, element_order, axis=1)
    phases = 2.0 * math.pi * frequency * delay_rows
    scaling = float(delays.shape[1]) ** (-0.5)
    cosines = jnp.cos(phases) * scaling
    sines = -jnp.sin(phases) * scaling
    upper_rows = jnp.concatenate([cosines.T, sines.T], axis=1)
    lower_rows = jnp.concatenate([-sines.T, cosines.T], axis=1)
    return jnp.concatenate([upper_rows, lower_rows], axis=0)


def project(arrived, weights):
    columns = arrived.shape[2]
    stacked = arrived.reshape(2 * arrived.shape[1], columns)
    return lax.dot_general(
        stacked,
        weights,
        (((0,), (0,)), ((), ())),
        precision=lax.Precision.HIGHEST,
        preferred_element_type=jnp.float32,
    )


def local(snapshots, delays, element_order, beam_table, band_len):
    unit_count = lax.axis_size("elem")
    position = lax.axis_index("elem")
    frequency, band_size, selector = band_of(band_len, position, unit_count)
    weights = steering(delays, element_order, beam_table, frequency)
    beam_count = beam_table.shape[0]
    local_elems = snapshots.shape[1]
    unit_cols = snapshots.shape[2] // unit_count
    divided = snapshots.reshape(2, local_elems, unit_count, unit_cols)
    pieces = lax.all_to_all(divided, "elem", split_axis=2, concat_axis=1, tiled=True)
    formed = project(pieces.reshape(2, pieces.shape[1], pieces.shape[3]), weights)
    column_count = formed.shape[0]
    squares = jnp.sum(formed * formed, axis=0)
    power_mean = (squares[:beam_count] + squares[beam_count:]) / (
        band_size.astype(jnp.float32) * column_count
    )
    partial_value = selector[:, None] * power_mean[None, :]
    summed = lax.psum(partial_value, "elem")
    decibels = 10.0 * jnp.log10(summed + epsilon)
    return (formed.reshape(column_count, 2, beam_count), decibels)


def solution(mesh):
    n = mesh.shape["elem"]
    body = functools.partial(local_ring, n) if fits(mesh) else local
    return jax.shard_map(
        body,
        mesh=mesh,
        in_specs=(P(None, ("groups", "elem"), None), P(), P("groups"), P("groups"), P()),
        out_specs=(P("elem", None, "groups"), P(None, "groups")),
        check_vma=False,
    )
```

```python
import functools
import math

import jax
import jax.numpy as jnp
from jax import lax
from jax.experimental import pallas as pl
from jax.experimental.pallas import tpu as pltpu
from jax.sharding import PartitionSpec as P

epsilon = 1e-06
SIDE = 2
RING = 4
CHUNKS = 8


def band_of(band_len, position, unit_count):
    band_ends = jnp.cumsum(band_len)
    band_index = jnp.sum((band_ends <= position).astype(jnp.int32))
    selector = jnp.arange(band_len.shape[0], dtype=jnp.int32) == band_index
    band_size = jnp.sum(jnp.where(selector, band_len, 0))
    band_start = jnp.sum(jnp.where(selector, band_ends, 0)) - band_size
    frequency = (band_start.astype(jnp.float32) + 0.5 * band_size.astype(jnp.float32)) / float(
        unit_count
    )
    return (frequency, band_size, selector.astype(jnp.float32))


def sincos(turns):
    reduced = turns - jnp.floor(turns + 0.5)
    x = reduced * math.pi
    q = x * x
    sin_terms = [(-1.0) ** i / math.factorial(2 * i + 1) for i in range(7)]
    cos_terms = [(-1.0) ** i / math.factorial(2 * i) for i in range(8)]
    s = jnp.full_like(q, sin_terms[-1])
    for term in sin_terms[-2::-1]:
        s = s * q + term
    s = s * x
    c = jnp.full_like(q, cos_terms[-1])
    for term in cos_terms[-2::-1]:
        c = c * q + term
    return 2.0 * s * c, 1.0 - 2.0 * s * s


def split2(v):
    high = v.astype(jnp.bfloat16)
    return high, (v - high.astype(jnp.float32)).astype(jnp.bfloat16)


def split3(v):
    high = v.astype(jnp.bfloat16)
    rest = v - high.astype(jnp.float32)
    middle = rest.astype(jnp.bfloat16)
    return high, middle, (rest - middle.astype(jnp.float32)).astype(jnp.bfloat16)


def item_unit(i):
    return 3 - i + (i + RING) // (RING + 1) + i // (RING + 1)


def item_chunk(i):
    return CHUNKS - 2 + (i + RING) // (RING + 1) - i // (RING + 1)


def kernel(
    n, lens, x, delays, order, table, out, power, bands,
    bl, dl, od, tb, g1, dt, wh, wl, xa, xb, xz, pa, pb, ra, rb, ry, fin, tot,
    in_s, own_a, own_b, sa_s, sa_r, sb_s, sb_r, sy_s, sy_r, sz_s, sz_r,
    a_s, a_r, b_s, b_r, y2_s, y2_r, f_s, f_r, p_s, p_r,
):
    me = lax.axis_index("elem")
    core = me % SIDE
    y = (me // SIDE) % SIDE
    z = me // (SIDE * SIDE)
    upper = z // 2
    end = z + upper * (RING - 1 - 2 * z)
    unit_cols = x.shape[2] // n
    chunk = unit_cols // CHUNKS
    most = CHUNKS - 1
    beams = table.shape[1]
    scaling = float(delays.shape[1]) ** (-0.5)
    slots = (3, 2, 1 - end, end)
    early = (most - 1, most, most - end, most - 1 + end)

    def chip(u):
        return u + upper * (RING - 1 - 2 * u)

    def dev(zz, yy, cc):
        return (zz * SIDE + yy % SIDE) * SIDE + cc % SIDE

    ahead = dev(chip(end + 1), y, core)
    beside = dev(chip(1 - end), y, core)

    barrier = pltpu.get_barrier_semaphore()

    def greet(target):
        pl.semaphore_signal(barrier, inc=1, device_id={"elem": target},
                            device_id_type=pl.DeviceIdType.MESH)

    for r in (0, 1):
        greet(dev(z, y + 1, core + r))
        greet(dev(chip(1 - end), y, core + r))
    greet(dev(z, y, core + 1))

    @pl.when(end == 1)
    def _():
        greet(ahead)

    fetches = [
        pltpu.make_async_copy(lens, bl, in_s.at[0]),
        pltpu.make_async_copy(delays, dl, in_s.at[1]),
        pltpu.make_async_copy(order, od, in_s.at[2]),
        pltpu.make_async_copy(table, tb, in_s.at[3]),
    ]
    for fetch in fetches:
        fetch.start()
    pl.semaphore_wait(barrier, 5 + end)

    def remote(src, dst, send, recv, target):
        return pltpu.make_async_remote_copy(
            src_ref=src, dst_ref=dst, send_sem=send, recv_sem=recv,
            device_id={"elem": target}, device_id_type=pl.DeviceIdType.MESH)

    def cols(unit, start, size):
        return x.at[:, :, pl.ds(pl.multiple_of(unit * unit_cols + start, 128), size)]

    def part(k):
        return pl.ds(pl.multiple_of(k * chunk, 128), chunk)

    def y_copy(j, k, r):
        return remote(
            cols(dev(chip(slots[j]), y + 1, core + r), k * chunk, chunk),
            xa.at[2 + r, j, :, :, part(k)],
            sy_s.at[r, j, k], sy_r.at[r, j, k], dev(z, y + 1, core + r))

    def late(i, yy, cc):
        return cols(dev(chip(item_unit(i)), yy, cc), item_chunk(i) * chunk, chunk)

    def z_copy(i, yr, r):
        return remote(
            late(i, y + yr, core + r), xz.at[i, r, yr],
            sz_s.at[i, r, yr], sz_r.at[i, r, yr], dev(chip(1 - end), y, core + r))

    def b_peer(i, yr):
        return remote(late(i, y + yr, core + 1), xb.at[1, i, yr],
                      sb_s.at[i, yr], sb_r.at[i, yr], dev(z, y, core + 1))

    def b_own(i, yr):
        return pltpu.make_async_copy(late(i, y + yr, core), xb.at[0, i, yr], own_b.at[i, yr])

    def a_copy(j, k):
        to = j + 3 * end if j < 2 else 2
        return remote(pa.at[j, k], ra.at[to, k], a_s.at[j, k], a_r.at[to, k],
                      ahead if j < 2 else beside)

    def a_wait(to, k):
        remote(pa.at[0, k], ra.at[to, k], a_s.at[0, k], a_r.at[to, k], beside).wait_recv()

    def b_ahead(i, yr):
        return remote(pb.at[i, yr], rb.at[i, yr], b_s.at[i, yr], b_r.at[i, yr], ahead)

    def b_back(i, yr):
        return remote(pb.at[i, yr], rb.at[i - 1, yr], b_s.at[i - 1, yr], b_r.at[i - 1, yr],
                      beside)

    def last(i):
        return remote(pb.at[i, 1], ry.at[i - 3], y2_s.at[i - 3], y2_r.at[i - 3],
                      dev(z, y + 1, core))

    half = beams // 2

    def quarter(b):
        return pl.ds(b * half, half)

    def y_final(b):
        return remote(pb.at[5, 1, quarter(b)], ry.at[2, quarter(b)],
                      f_s.at[0, b], f_r.at[0, b], dev(z, y + 1, core))

    def z_final(b):
        return remote(pa.at[2, most - 1, quarter(b)], ra.at[2, most - 1, quarter(b)],
                      f_s.at[1, b], f_r.at[1, b], beside)

    def every(low, high, step):
        def body(t, carry):
            step(t)
            return carry

        lax.fori_loop(low, high, body, 0)

    pairs = [(yr, r) for yr in (1, 0) for r in (0, 1)]

    def issue():
        def start(k):
            for r in (0, 1):
                y_copy(0, k, r).start()

        every(1, early[0], start)

        @pl.when(end == 0)
        def _():
            def start(t):
                for r in (0, 1):
                    z_copy(t // 2, 1 - t % 2, r).start()

            every(1, 8, start)

        for j in (1, 2, 3):
            def start(k, j=j):
                for r in (0, 1):
                    y_copy(j, k, r).start()

            every(0, early[j], start)

    y_copy(0, 0, 0).start()

    @pl.when(end == 0)
    def _():
        z_copy(0, 1, 0).start()

    def rest():
        y_copy(0, 0, 1).start()

        @pl.when(end == 0)
        def _():
            z_copy(0, 1, 1).start()

        issue()

    @pl.when(core == 0)
    def _():
        rest()

    ca, la = {}, {}

    def b_start(i):
        for yr in (1, 0):
            b_peer(i, yr).start()
            b_own(i, yr).start()

    for j in range(4):
        there = dev(chip(slots[j]), y, core + 1)
        here = dev(chip(slots[j]), y, core)
        ca[j] = remote(cols(there, 0, most * chunk), xa.at[1, j],
                       sa_s.at[j], sa_r.at[j], dev(z, y, core + 1))
        la[j] = pltpu.make_async_copy(cols(here, 0, most * chunk), xa.at[0, j], own_a.at[j])
        ca[j].start()
        la[j].start()
        if j == 0:
            every(4 - 4 * end, 6, b_start)

    for fetch in fetches:
        fetch.wait()

    def frequency(unit):
        total, value = 0, 0.0
        for b in range(lens.shape[0]):
            size = bl[b]
            inside = jnp.logical_and(unit >= total, unit < total + size)
            middle = (2 * total + size).astype(jnp.float32) * (0.5 / n)
            value = jnp.where(inside, middle, value)
            total = total + size
        return value

    band = lax.broadcasted_iota(jnp.int32, bands.shape[1:], 0)
    total = 0
    for b in range(lens.shape[0]):
        bands[0] = jnp.where(band == b, total, bands[0] if b else 0)
        bands[1] = jnp.where(band == b, bl[b], bands[1] if b else 0)
        total = total + bl[b]

    beam_hot = jnp.where(
        lax.broadcasted_iota(jnp.int32, (delays.shape[0], beams), 0) == tb[...], 1.0, 0.0
    ).T.astype(jnp.bfloat16)
    step = 512 if delays.shape[1] % 512 == 0 else delays.shape[1]

    def pick_beams(i):
        span = pl.ds(pl.multiple_of(i * step, step), step)
        parts = split3(dl[:, span])
        rows = [jnp.dot(beam_hot, piece, preferred_element_type=jnp.float32) for piece in parts]
        for m, piece in enumerate(rows):
            g1[m * beams:(m + 1) * beams, span] = piece.astype(jnp.bfloat16)

    every(0, delays.shape[1] // step, pick_beams)

    def pick_elems(s):
        r, g = s % 2, s // 2
        u = end + (g // 2) * (1 - 2 * end)
        q = dev(chip(u), y + g % 2, core + r)
        row = od[q]
        hot = jnp.where(
            lax.broadcasted_iota(jnp.int32, (delays.shape[1], row.shape[1]), 0) == row, 1.0, 0.0
        ).astype(jnp.bfloat16)
        got = jnp.dot(g1[...], hot, preferred_element_type=jnp.float32)
        dt[s] = got[:beams] + got[beams:2 * beams] + got[2 * beams:]

    every(0, 1, pick_elems)

    @pl.when(core == 1)
    def _():
        rest()

    every(1, 6, pick_elems)
    wide = 2 * x.shape[1]

    def weigh(f, sources):
        for i, s in enumerate(sources):
            sine, cosine = sincos(f * dt[s])
            ch, cl = split2(cosine * scaling)
            sh, sl = split2(sine * scaling)
            span = slice(i * wide, (i + 1) * wide)
            wh[:beams, span] = jnp.concatenate([ch, sh], axis=1)
            wh[beams:, span] = jnp.concatenate([-sh, ch], axis=1)
            wl[:beams, span] = jnp.concatenate([cl, sl], axis=1)
            wl[beams:, span] = jnp.concatenate([-sl, cl], axis=1)

    def form(pieces):
        rows = jnp.concatenate([piece.reshape(wide, chunk) for piece in pieces], axis=0)
        xh, xl = split2(rows)
        span = slice(0, wide * len(pieces))
        dot = functools.partial(jnp.dot, preferred_element_type=jnp.float32)
        high = wh[:, span]
        return dot(high, xh) + (dot(high, xl) + dot(wl[:, span], xh))

    def a_slot(j, then, pause=None):
        weigh(frequency(dev(chip(slots[j]), y, core)), (0, 1, 2, 3))
        la[j].wait()
        ca[j].wait_recv()

        def one(k):
            for r in (0, 1):
                y_copy(j, k, r).wait_recv()
            pa[j, k] = form([xa[s, j, :, :, part(k)] for s in range(4)])
            then(k)

        if pause is None:
            every(0, early[j], one)
        else:
            every(0, early[j] - 1, one)
            pause()
            one(early[j] - 1)

    def join(j, to, k):
        a_wait(to, k)
        pa[j, k] += ra[to, k]

    def after0(k):
        @pl.when(end == 0)
        def _():
            a_copy(0, k).start()

    def join0(k):
        join(0, 0, k)
        a_copy(0, k).start()

    def join1(k):
        join(1, 1, k)
        a_copy(1, k).start()

    def after1(k):
        @pl.when(end == 0)
        def _():
            a_copy(1, k).start()

        @pl.when(jnp.logical_and(end == 1, k < early[0]))
        def _():
            join0(k)

    def after2(k):
        @pl.when(end == 1)
        def _():
            join(2, 3, k)

        @pl.when(k < most - 1)
        def _():
            a_copy(2, k).start()

        @pl.when(k == most - 1)
        def _():
            for b in (0, 2, 1, 3):
                z_final(b).start()

        @pl.when(end == 1)
        def _():
            join1(k)

    def put(got, start):
        rows = pl.ds(pl.multiple_of(start, 128), chunk)
        out[rows, 0, :] = got[:, :beams]
        out[rows, 1, :] = got[:, beams:]

    def emit(got, start):
        put(got, start)
        tot[...] += jnp.sum(got * got, axis=0, keepdims=True)

    def after3(k):
        @pl.when(end == 1)
        def _():
            join(3, 4, k)

        @pl.when(k < most - 1)
        def _():
            a_wait(2, k)
            emit((pa[3, k] + ra[2, k]).T, k * chunk)

    tot[...] = jnp.zeros_like(tot)

    def b_landed(i, yr):
        b_own(i, yr).wait()
        b_peer(i, yr).wait_recv()

    def b_joint(i, yr):
        for r in (0, 1):
            z_copy(i, yr, r).wait_recv()
        b_landed(i, yr)
        weigh(frequency(dev(chip(item_unit(i)), y + yr, core)), (0, 1, 4, 5))
        pb[i, yr] = form([xb[0, i, yr], xb[1, i, yr], xz[i, 0, yr], xz[i, 1, yr]])

    @pl.when(end == 1)
    def _():
        def b_first(t):
            i, yr = t // 2, 1 - t % 2
            b_joint(i, yr)
            b_ahead(i, yr).start()

        every(0, 6, b_first)

    a_slot(0, after0)

    def b_end(t):
        i, yr = 4 + t % 2, 1 - t // 2
        b_landed(i, yr)
        weigh(frequency(dev(chip(0), y + yr, core)), (0, 1))
        pb[i, yr] = form([xb[0, i, yr], xb[1, i, yr]])

    every(0, 4, b_end)
    a_slot(1, after1)

    @pl.when(end == 1)
    def _():
        for i in range(2):
            for yr in (1, 0):
                b_ahead(i, yr).wait_recv()
                pb[5 - i, yr] += rb[i, yr]
                b_back(5 - i, yr).start()

        def b_home(t):
            yr = 1 - t
            b_joint(3, yr)
            b_ahead(2, yr).wait_recv()
            pb[3, yr] += rb[2, yr]

        every(0, 2, b_home)

    a_slot(2, after2)

    @pl.when(end == 1)
    def _():
        join1(most - 1)
        last(3).start()

    @pl.when(end == 0)
    def _():
        for i in (4, 5):
            for yr in (1, 0):
                b_back(i, yr).wait_recv()
                pb[i, yr] += rb[i - 1, yr]
        last(4).start()
        for b in (0, 2, 1, 3):
            y_final(b).start()

    def finish(i):
        last(i).wait_recv()
        emit((pb[i, 0] + ry[i - 3]).T, item_chunk(i) * chunk)

    a_slot(3, after3, lambda: every(3, 3 + end, finish))

    @pl.when(end == 0)
    def _():
        finish(4)

    early_power = tot[:, :beams] + tot[:, beams:]
    for p in (0, 1):
        @pl.when(end == 0)
        def _():
            for b in (p, p + 2):
                y_final(b).wait_recv()
                fin[quarter(b)] = pb[5, 0, quarter(b)] + ry[2, quarter(b)]

        @pl.when(end == 1)
        def _():
            for b in (p, p + 2):
                z_final(b).wait_recv()
                fin[quarter(b)] = pa[3, most - 1, quarter(b)] + ra[2, most - 1, quarter(b)]

        real, imag = fin[quarter(p)], fin[quarter(p + 2)]
        late_row = jnp.sum((real * real + imag * imag).T, axis=0, keepdims=True)
        power[me, :, quarter(p)] = early_power[:, p * half:(p + 1) * half] + late_row

    def p_copy(target):
        return remote(power.at[me], power.at[me], p_s, p_r, target)

    def p_far(t):
        p_copy(dev(chip(3 - t // (SIDE * SIDE)), y + 1 + t // SIDE, core + t)).start()

    others = 3 - end
    every(0, others * SIDE * SIDE, p_far)

    @pl.when(end == 1)
    def _():
        for t in range(SIDE * SIDE):
            p_copy(dev(chip(0), y + 1 + t // SIDE, core + t)).start()

    for t in range(SIDE * SIDE - 1):
        p_copy(dev(z, y + 1 + t // SIDE, core + t + t // SIDE)).start()

    put(fin[...].T, (most - 1) * chunk)

    def last_sent(i):
        last(i).wait_send()

    every(4 - end, 5 - end, last_sent)

    @pl.when(end == 0)
    def _():
        for b in range(4):
            y_final(b).wait_send()
            z_final(b).wait_send()

    def b_sent(i):
        for yr in (1, 0):
            b_peer(i, yr).wait_send()

    every(4 - 4 * end, 6, b_sent)
    for j in range(4):
        ca[j].wait_send()

        def drain(k, j=j):
            for r in (0, 1):
                y_copy(j, k, r).wait_send()
            if j < 2:
                a_copy(j, k).wait_send()

        every(0, early[j], drain)

    every(0, most - 1, lambda k: a_copy(2, k).wait_send())

    @pl.when(end == 0)
    def _():
        def z_sent(i):
            for yr, r in pairs:
                z_copy(i, yr, r).wait_send()

        every(0, 4, z_sent)

    @pl.when(end == 1)
    def _():
        for yr in (1, 0):
            for i in range(3):
                b_ahead(i, yr).wait_send()
            for i in (4, 5):
                b_back(i, yr).wait_send()

    rest = power.at[pl.ds(0, n - 1)]
    remote(rest, rest, p_s, p_r, beside).wait()


def conclude(n, formed, power, bands, beams, decibels, level, sems):
    pieces = sems.shape[0] - 1
    rows = formed.shape[0] // pieces
    copies = []
    for i in range(pieces):
        span = pl.ds(i * rows, rows)
        copies.append(pltpu.make_async_copy(formed.at[span], beams.at[span], sems.at[i]))
        copies[-1].start()
    low, size = bands[0], bands[1]
    high = low + size
    summed = jnp.zeros(level.shape, jnp.float32)
    for u in range(n):
        inside = jnp.logical_and(low <= u, u < high)
        summed = summed + jnp.where(inside, power[u], 0.0)
    mean = summed / (size.astype(jnp.float32) * formed.shape[0])
    level[...] = (10.0 / math.log(10.0)) * jnp.log(mean + epsilon)
    copies.append(pltpu.make_async_copy(level, decibels, sems.at[pieces]))
    copies[-1].start()
    for copy in copies:
        copy.wait()


def local_ring(n, snapshots, delays, element_order, beam_table, band_len):
    local_elems = snapshots.shape[1]
    unit_cols = snapshots.shape[2] // n
    beams = beam_table.shape[0]
    most, chunk = CHUNKS - 1, unit_cols // CHUNKS
    block = (2 * beams, chunk)
    f32, sem = jnp.float32, pltpu.SemaphoreType.DMA
    raw = (2, local_elems)
    vmem, hbm = (pl.BlockSpec(memory_space=m) for m in (pltpu.VMEM, pl.ANY))
    band_shape = (band_len.shape[0], beams)
    formed, power, bands = pl.pallas_call(
        functools.partial(kernel, n),
        out_shape=(
            pltpu.VMEM((unit_cols, 2, beams), f32),
            pltpu.VMEM((n, 1, beams), f32),
            pltpu.VMEM((2,) + band_shape, jnp.int32),
        ),
        in_specs=[hbm] * 5,
        out_specs=(vmem, vmem, vmem),
        scratch_shapes=[
            pltpu.SMEM(band_len.shape, jnp.int32),
            pltpu.VMEM(delays.shape, f32),
            pltpu.VMEM((n, 1, local_elems), jnp.int32),
            pltpu.VMEM((1, beams), jnp.int32),
            pltpu.VMEM((3 * beams, delays.shape[1]), jnp.bfloat16),
            pltpu.VMEM((6, beams, local_elems), f32),
            pltpu.VMEM((2 * beams, 8 * local_elems), jnp.bfloat16),
            pltpu.VMEM((2 * beams, 8 * local_elems), jnp.bfloat16),
            pltpu.VMEM((4, 4) + raw + (most * chunk,), f32),
            pltpu.VMEM((2, 6, 2) + raw + (chunk,), f32),
            pltpu.VMEM((4, 2, 2) + raw + (chunk,), f32),
            pltpu.VMEM((4, most) + block, f32),
            pltpu.VMEM((6, 2) + block, f32),
            pltpu.VMEM((5, most) + block, f32),
            pltpu.VMEM((5, 2) + block, f32),
            pltpu.VMEM((3,) + block, f32),
            pltpu.VMEM(block, f32),
            pltpu.VMEM((1, 2 * beams), f32),
            sem((4,)), sem((4,)), sem((6, 2)),
            sem((4,)), sem((4,)), sem((6, 2)), sem((6, 2)),
            sem((2, 4, most)), sem((2, 4, most)), sem((4, 2, 2)), sem((4, 2, 2)),
            sem((3, most)), sem((5, most)), sem((5, 2)), sem((5, 2)),
            sem((3,)), sem((3,)),
            sem((2, 4)), sem((2, 4)),
            sem, sem,
        ],
        compiler_params=pltpu.CompilerParams(
            collective_id=0, has_side_effects=True, vmem_limit_bytes=54 * 1024 * 1024
        ),
    )(
        band_len, snapshots, delays,
        element_order.reshape(n, 1, local_elems), beam_table.reshape(1, beams),
    )
    parts = [pltpu.with_memory_space_constraint(v, pltpu.VMEM) for v in (formed, power, bands)]
    return pl.pallas_call(
        functools.partial(conclude, n),
        out_shape=(
            jax.ShapeDtypeStruct((unit_cols, 2, beams), f32),
            jax.ShapeDtypeStruct(band_shape, f32),
        ),
        in_specs=[vmem] * 3,
        out_specs=(hbm, hbm),
        scratch_shapes=[pltpu.VMEM(band_shape, f32), sem((9,))],
    )(*parts)


def fits(mesh):
    return mesh.shape["elem"] == SIDE * SIDE * RING


def steering(delays, element_order, beam_table, frequency):
    delay_rows = jnp.take(delays, beam_table, axis=0)
    delay_rows = jnp.take(delay_rows, element_order, axis=1)
    phases = 2.0 * math.pi * frequency * delay_rows
    scaling = float(delays.shape[1]) ** (-0.5)
    cosines = jnp.cos(phases) * scaling
    sines = -jnp.sin(phases) * scaling
    upper_rows = jnp.concatenate([cosines.T, sines.T], axis=1)
    lower_rows = jnp.concatenate([-sines.T, cosines.T], axis=1)
    return jnp.concatenate([upper_rows, lower_rows], axis=0)


def project(arrived, weights):
    columns = arrived.shape[2]
    stacked = arrived.reshape(2 * arrived.shape[1], columns)
    return lax.dot_general(
        stacked,
        weights,
        (((0,), (0,)), ((), ())),
        precision=lax.Precision.HIGHEST,
        preferred_element_type=jnp.float32,
    )


def local(snapshots, delays, element_order, beam_table, band_len):
    unit_count = lax.axis_size("elem")
    position = lax.axis_index("elem")
    frequency, band_size, selector = band_of(band_len, position, unit_count)
    weights = steering(delays, element_order, beam_table, frequency)
    beam_count = beam_table.shape[0]
    local_elems = snapshots.shape[1]
    unit_cols = snapshots.shape[2] // unit_count
    divided = snapshots.reshape(2, local_elems, unit_count, unit_cols)
    pieces = lax.all_to_all(divided, "elem", split_axis=2, concat_axis=1, tiled=True)
    formed = project(pieces.reshape(2, pieces.shape[1], pieces.shape[3]), weights)
    column_count = formed.shape[0]
    squares = jnp.sum(formed * formed, axis=0)
    power_mean = (squares[:beam_count] + squares[beam_count:]) / (
        band_size.astype(jnp.float32) * column_count
    )
    partial_value = selector[:, None] * power_mean[None, :]
    summed = lax.psum(partial_value, "elem")
    decibels = 10.0 * jnp.log10(summed + epsilon)
    return (formed.reshape(column_count, 2, beam_count), decibels)


def solution(mesh):
    n = mesh.shape["elem"]
    body = functools.partial(local_ring, n) if fits(mesh) else local
    return jax.shard_map(
        body,
        mesh=mesh,
        in_specs=(P(None, ("groups", "elem"), None), P(), P("groups"), P("groups"), P()),
        out_specs=(P("elem", None, "groups"), P(None, "groups")),
        check_vma=False,
    )
```

```python
import functools
import math

import jax
import jax.numpy as jnp
from jax import lax
from jax.experimental import pallas as pl
from jax.experimental.pallas import tpu as pltpu
from jax.sharding import PartitionSpec as P

epsilon = 1e-06
SIDE = 2
RING = 4
CHUNKS = 8


def band_of(band_len, position, unit_count):
    band_ends = jnp.cumsum(band_len)
    band_index = jnp.sum((band_ends <= position).astype(jnp.int32))
    selector = jnp.arange(band_len.shape[0], dtype=jnp.int32) == band_index
    band_size = jnp.sum(jnp.where(selector, band_len, 0))
    band_start = jnp.sum(jnp.where(selector, band_ends, 0)) - band_size
    frequency = (band_start.astype(jnp.float32) + 0.5 * band_size.astype(jnp.float32)) / float(
        unit_count
    )
    return (frequency, band_size, selector.astype(jnp.float32))


def sincos(turns):
    reduced = turns - jnp.floor(turns + 0.5)
    x = reduced * math.pi
    q = x * x
    sin_terms = [(-1.0) ** i / math.factorial(2 * i + 1) for i in range(7)]
    cos_terms = [(-1.0) ** i / math.factorial(2 * i) for i in range(8)]
    s = jnp.full_like(q, sin_terms[-1])
    for term in sin_terms[-2::-1]:
        s = s * q + term
    s = s * x
    c = jnp.full_like(q, cos_terms[-1])
    for term in cos_terms[-2::-1]:
        c = c * q + term
    return 2.0 * s * c, 1.0 - 2.0 * s * s


def split2(v):
    high = v.astype(jnp.bfloat16)
    return high, (v - high.astype(jnp.float32)).astype(jnp.bfloat16)


def split3(v):
    high = v.astype(jnp.bfloat16)
    rest = v - high.astype(jnp.float32)
    middle = rest.astype(jnp.bfloat16)
    return high, middle, (rest - middle.astype(jnp.float32)).astype(jnp.bfloat16)


def item_unit(i):
    return 3 - i + (i + RING) // (RING + 1) + i // (RING + 1)


def item_chunk(i):
    return CHUNKS - 2 + (i + RING) // (RING + 1) - i // (RING + 1)


def kernel(
    n, lens, x, delays, order, table, out, power, bands,
    bl, dl, od, tb, g1, dt, wh, wl, xa, xb, xz, pa, pb, ra, rb, ry, fin, tot,
    in_s, own_a, own_b, sa_s, sa_r, sb_s, sb_r, sy_s, sy_r, sz_s, sz_r,
    a_s, a_r, b_s, b_r, y2_s, y2_r, f_s, f_r, p_s, p_r,
):
    me = lax.axis_index("elem")
    core = me % SIDE
    y = (me // SIDE) % SIDE
    z = me // (SIDE * SIDE)
    upper = z // 2
    end = z + upper * (RING - 1 - 2 * z)
    unit_cols = x.shape[2] // n
    chunk = unit_cols // CHUNKS
    most = CHUNKS - 1
    beams = table.shape[1]
    scaling = float(delays.shape[1]) ** (-0.5)
    slots = (3, 2, 1 - end, end)
    early = (most - 1, most, most - end, most - 1 + end)

    def chip(u):
        return u + upper * (RING - 1 - 2 * u)

    def dev(zz, yy, cc):
        return (zz * SIDE + yy % SIDE) * SIDE + cc % SIDE

    ahead = dev(chip(end + 1), y, core)
    beside = dev(chip(1 - end), y, core)

    barrier = pltpu.get_barrier_semaphore()

    def greet(target):
        pl.semaphore_signal(barrier, inc=1, device_id={"elem": target},
                            device_id_type=pl.DeviceIdType.MESH)

    for r in (1, 0):
        greet(dev(z, y + 1, core + r))
    for r in (1, 0):
        greet(dev(chip(1 - end), y, core + r))
    greet(dev(z, y, core + 1))

    @pl.when(end == 1)
    def _():
        greet(ahead)

    fetches = [
        pltpu.make_async_copy(lens, bl, in_s.at[0]),
        pltpu.make_async_copy(delays, dl, in_s.at[1]),
        pltpu.make_async_copy(order, od, in_s.at[2]),
        pltpu.make_async_copy(table, tb, in_s.at[3]),
    ]
    for fetch in fetches:
        fetch.start()
    pl.semaphore_wait(barrier, 5 + end)

    def remote(src, dst, send, recv, target):
        return pltpu.make_async_remote_copy(
            src_ref=src, dst_ref=dst, send_sem=send, recv_sem=recv,
            device_id={"elem": target}, device_id_type=pl.DeviceIdType.MESH)

    def cols(unit, start, size):
        return x.at[:, :, pl.ds(pl.multiple_of(unit * unit_cols + start, 128), size)]

    def part(k):
        return pl.ds(pl.multiple_of(k * chunk, 128), chunk)

    def y_copy(j, k, r):
        return remote(
            cols(dev(chip(slots[j]), y + 1, core + r), k * chunk, chunk),
            xa.at[2 + r, j, :, :, part(k)],
            sy_s.at[r, j, k], sy_r.at[r, j, k], dev(z, y + 1, core + r))

    def late(i, yy, cc):
        return cols(dev(chip(item_unit(i)), yy, cc), item_chunk(i) * chunk, chunk)

    def z_copy(i, yr, r):
        return remote(
            late(i, y + yr, core + r), xz.at[i, r, yr],
            sz_s.at[i, r, yr], sz_r.at[i, r, yr], dev(chip(1 - end), y, core + r))

    def b_peer(i, yr):
        return remote(late(i, y + yr, core + 1), xb.at[1, i, yr],
                      sb_s.at[i, yr], sb_r.at[i, yr], dev(z, y, core + 1))

    def b_own(i, yr):
        return pltpu.make_async_copy(late(i, y + yr, core), xb.at[0, i, yr], own_b.at[i, yr])

    def a_copy(j, k):
        to = j + 3 * end if j < 2 else 2
        return remote(pa.at[j, k], ra.at[to, k], a_s.at[j, k], a_r.at[to, k],
                      ahead if j < 2 else beside)

    def a_wait(to, k):
        remote(pa.at[0, k], ra.at[to, k], a_s.at[0, k], a_r.at[to, k], beside).wait_recv()

    def b_ahead(i, yr):
        return remote(pb.at[i, yr], rb.at[i, yr], b_s.at[i, yr], b_r.at[i, yr], ahead)

    def b_back(i, yr):
        return remote(pb.at[i, yr], rb.at[i - 1, yr], b_s.at[i - 1, yr], b_r.at[i - 1, yr],
                      beside)

    def last(i):
        return remote(pb.at[i, 1], ry.at[i - 3], y2_s.at[i - 3], y2_r.at[i - 3],
                      dev(z, y + 1, core))

    half = beams // 2

    def quarter(b):
        return pl.ds(b * half, half)

    def y_final(b):
        return remote(pb.at[5, 1, quarter(b)], ry.at[2, quarter(b)],
                      f_s.at[0, b], f_r.at[0, b], dev(z, y + 1, core))

    def z_final(b):
        return remote(pa.at[2, most - 1, quarter(b)], ra.at[2, most - 1, quarter(b)],
                      f_s.at[1, b], f_r.at[1, b], beside)

    def every(low, high, step):
        def body(t, carry):
            step(t)
            return carry

        lax.fori_loop(low, high, body, 0)

    pairs = [(yr, r) for yr in (1, 0) for r in (0, 1)]

    def issue():
        def start(k):
            for r in (0, 1):
                y_copy(0, k, r).start()

        every(1, early[0], start)

        @pl.when(end == 0)
        def _():
            def start(t):
                for r in (0, 1):
                    z_copy(t // 2, 1 - t % 2, r).start()

            every(1, 8, start)

        for j in (1, 2, 3):
            def start(k, j=j):
                for r in (0, 1):
                    y_copy(j, k, r).start()

            every(0, early[j], start)

    y_copy(0, 0, 0).start()

    @pl.when(end == 0)
    def _():
        z_copy(0, 1, 0).start()

    def rest():
        y_copy(0, 0, 1).start()

        @pl.when(end == 0)
        def _():
            z_copy(0, 1, 1).start()

        issue()

    @pl.when(core == 0)
    def _():
        rest()

    ca, la = {}, {}

    def b_start(i):
        for yr in (1, 0):
            b_peer(i, yr).start()
            b_own(i, yr).start()

    for j in range(4):
        there = dev(chip(slots[j]), y, core + 1)
        here = dev(chip(slots[j]), y, core)
        ca[j] = remote(cols(there, 0, most * chunk), xa.at[1, j],
                       sa_s.at[j], sa_r.at[j], dev(z, y, core + 1))
        la[j] = pltpu.make_async_copy(cols(here, 0, most * chunk), xa.at[0, j], own_a.at[j])
        ca[j].start()
        la[j].start()
        if j == 0:
            every(4 - 4 * end, 6, b_start)

    for fetch in fetches:
        fetch.wait()

    def frequency(unit):
        total, value = 0, 0.0
        for b in range(lens.shape[0]):
            size = bl[b]
            inside = jnp.logical_and(unit >= total, unit < total + size)
            middle = (2 * total + size).astype(jnp.float32) * (0.5 / n)
            value = jnp.where(inside, middle, value)
            total = total + size
        return value

    band = lax.broadcasted_iota(jnp.int32, bands.shape[1:], 0)
    total = 0
    for b in range(lens.shape[0]):
        bands[0] = jnp.where(band == b, total, bands[0] if b else 0)
        bands[1] = jnp.where(band == b, bl[b], bands[1] if b else 0)
        total = total + bl[b]

    beam_hot = jnp.where(
        lax.broadcasted_iota(jnp.int32, (delays.shape[0], beams), 0) == tb[...], 1.0, 0.0
    ).T.astype(jnp.bfloat16)
    step = 512 if delays.shape[1] % 512 == 0 else delays.shape[1]

    def pick_beams(i):
        span = pl.ds(pl.multiple_of(i * step, step), step)
        parts = split3(dl[:, span])
        rows = [jnp.dot(beam_hot, piece, preferred_element_type=jnp.float32) for piece in parts]
        for m, piece in enumerate(rows):
            g1[m * beams:(m + 1) * beams, span] = piece.astype(jnp.bfloat16)

    every(0, delays.shape[1] // step, pick_beams)

    def pick_elems(s):
        r, g = s % 2, s // 2
        u = end + (g // 2) * (1 - 2 * end)
        q = dev(chip(u), y + g % 2, core + r)
        row = od[q]
        hot = jnp.where(
            lax.broadcasted_iota(jnp.int32, (delays.shape[1], row.shape[1]), 0) == row, 1.0, 0.0
        ).astype(jnp.bfloat16)
        got = jnp.dot(g1[...], hot, preferred_element_type=jnp.float32)
        dt[s] = got[:beams] + got[beams:2 * beams] + got[2 * beams:]

    every(0, 1, pick_elems)

    @pl.when(core == 1)
    def _():
        rest()

    every(1, 6, pick_elems)
    wide = 2 * x.shape[1]

    def weigh(f, sources):
        for i, s in enumerate(sources):
            sine, cosine = sincos(f * dt[s])
            ch, cl = split2(cosine * scaling)
            sh, sl = split2(sine * scaling)
            span = slice(i * wide, (i + 1) * wide)
            wh[:beams, span] = jnp.concatenate([ch, sh], axis=1)
            wh[beams:, span] = jnp.concatenate([-sh, ch], axis=1)
            wl[:beams, span] = jnp.concatenate([cl, sl], axis=1)
            wl[beams:, span] = jnp.concatenate([-sl, cl], axis=1)

    def form(pieces):
        rows = jnp.concatenate([piece.reshape(wide, chunk) for piece in pieces], axis=0)
        xh, xl = split2(rows)
        span = slice(0, wide * len(pieces))
        dot = functools.partial(jnp.dot, preferred_element_type=jnp.float32)
        high = wh[:, span]
        return dot(high, xh) + (dot(high, xl) + dot(wl[:, span], xh))

    def a_slot(j, then, pause=None):
        weigh(frequency(dev(chip(slots[j]), y, core)), (0, 1, 2, 3))
        la[j].wait()
        ca[j].wait_recv()

        def one(k):
            for r in (0, 1):
                y_copy(j, k, r).wait_recv()
            pa[j, k] = form([xa[s, j, :, :, part(k)] for s in range(4)])
            then(k)

        if pause is None:
            every(0, early[j], one)
        else:
            every(0, early[j] - 1, one)
            pause()
            one(early[j] - 1)

    def join(j, to, k):
        a_wait(to, k)
        pa[j, k] += ra[to, k]

    def after0(k):
        @pl.when(end == 0)
        def _():
            a_copy(0, k).start()

    def join0(k):
        join(0, 0, k)
        a_copy(0, k).start()

    def join1(k):
        join(1, 1, k)
        a_copy(1, k).start()

    def after1(k):
        @pl.when(end == 0)
        def _():
            a_copy(1, k).start()

        @pl.when(jnp.logical_and(end == 1, k < early[0]))
        def _():
            join0(k)

    def after2(k):
        @pl.when(end == 1)
        def _():
            join(2, 3, k)

        @pl.when(k < most - 1)
        def _():
            a_copy(2, k).start()

        @pl.when(k == most - 1)
        def _():
            for b in (0, 2, 1, 3):
                z_final(b).start()

        @pl.when(end == 1)
        def _():
            join1(k)

    def put(got, start):
        rows = pl.ds(pl.multiple_of(start, 128), chunk)
        out[rows, 0, :] = got[:, :beams]
        out[rows, 1, :] = got[:, beams:]

    def emit(got, start):
        put(got, start)
        tot[...] += jnp.sum(got * got, axis=0, keepdims=True)

    def after3(k):
        @pl.when(end == 1)
        def _():
            join(3, 4, k)

        @pl.when(k < most - 1)
        def _():
            a_wait(2, k)
            emit((pa[3, k] + ra[2, k]).T, k * chunk)

    tot[...] = jnp.zeros_like(tot)

    def b_landed(i, yr):
        b_own(i, yr).wait()
        b_peer(i, yr).wait_recv()

    def b_joint(i, yr):
        for r in (0, 1):
            z_copy(i, yr, r).wait_recv()
        b_landed(i, yr)
        weigh(frequency(dev(chip(item_unit(i)), y + yr, core)), (0, 1, 4, 5))
        pb[i, yr] = form([xb[0, i, yr], xb[1, i, yr], xz[i, 0, yr], xz[i, 1, yr]])

    @pl.when(end == 1)
    def _():
        def b_first(t):
            i, yr = t // 2, 1 - t % 2
            b_joint(i, yr)
            b_ahead(i, yr).start()

        every(0, 6, b_first)

    a_slot(0, after0)

    def b_end(t):
        i, yr = 4 + t % 2, 1 - t // 2
        b_landed(i, yr)
        weigh(frequency(dev(chip(0), y + yr, core)), (0, 1))
        pb[i, yr] = form([xb[0, i, yr], xb[1, i, yr]])

    every(0, 4, b_end)
    a_slot(1, after1)

    @pl.when(end == 1)
    def _():
        for i in range(2):
            for yr in (1, 0):
                b_ahead(i, yr).wait_recv()
                pb[5 - i, yr] += rb[i, yr]
                b_back(5 - i, yr).start()

        def b_home(t):
            yr = 1 - t
            b_joint(3, yr)
            b_ahead(2, yr).wait_recv()
            pb[3, yr] += rb[2, yr]

        every(0, 2, b_home)

    a_slot(2, after2)

    @pl.when(end == 1)
    def _():
        join1(most - 1)
        last(3).start()

    @pl.when(end == 0)
    def _():
        for i in (4, 5):
            for yr in (1, 0):
                b_back(i, yr).wait_recv()
                pb[i, yr] += rb[i - 1, yr]
        last(4).start()
        for b in (0, 2, 1, 3):
            y_final(b).start()

    def finish(i):
        last(i).wait_recv()
        emit((pb[i, 0] + ry[i - 3]).T, item_chunk(i) * chunk)

    a_slot(3, after3, lambda: every(3, 3 + end, finish))

    @pl.when(end == 0)
    def _():
        finish(4)

    early_power = tot[:, :beams] + tot[:, beams:]
    for p in (0, 1):
        @pl.when(end == 0)
        def _():
            for b in (p, p + 2):
                y_final(b).wait_recv()
                fin[quarter(b)] = pb[5, 0, quarter(b)] + ry[2, quarter(b)]

        @pl.when(end == 1)
        def _():
            for b in (p, p + 2):
                z_final(b).wait_recv()
                fin[quarter(b)] = pa[3, most - 1, quarter(b)] + ra[2, most - 1, quarter(b)]

        real, imag = fin[quarter(p)], fin[quarter(p + 2)]
        late_row = jnp.sum((real * real + imag * imag).T, axis=0, keepdims=True)
        power[me, :, quarter(p)] = early_power[:, p * half:(p + 1) * half] + late_row

    def p_copy(target):
        return remote(power.at[me], power.at[me], p_s, p_r, target)

    def p_far(t):
        p_copy(dev(chip(3 - t // (SIDE * SIDE)), y + 1 + t // SIDE, core + t)).start()

    others = 3 - end
    every(0, others * SIDE * SIDE, p_far)

    @pl.when(end == 1)
    def _():
        for t in range(SIDE * SIDE):
            p_copy(dev(chip(0), y + 1 + t // SIDE, core + t)).start()

    for t in range(SIDE * SIDE - 1):
        p_copy(dev(z, y + 1 + t // SIDE, core + t + t // SIDE)).start()

    put(fin[...].T, (most - 1) * chunk)

    def last_sent(i):
        last(i).wait_send()

    every(4 - end, 5 - end, last_sent)

    @pl.when(end == 0)
    def _():
        for b in range(4):
            y_final(b).wait_send()
            z_final(b).wait_send()

    def b_sent(i):
        for yr in (1, 0):
            b_peer(i, yr).wait_send()

    every(4 - 4 * end, 6, b_sent)
    for j in range(4):
        ca[j].wait_send()

        def drain(k, j=j):
            for r in (0, 1):
                y_copy(j, k, r).wait_send()
            if j < 2:
                a_copy(j, k).wait_send()

        every(0, early[j], drain)

    every(0, most - 1, lambda k: a_copy(2, k).wait_send())

    @pl.when(end == 0)
    def _():
        def z_sent(i):
            for yr, r in pairs:
                z_copy(i, yr, r).wait_send()

        every(0, 4, z_sent)

    @pl.when(end == 1)
    def _():
        for yr in (1, 0):
            for i in range(3):
                b_ahead(i, yr).wait_send()
            for i in (4, 5):
                b_back(i, yr).wait_send()

    rest = power.at[pl.ds(0, n - 1)]
    remote(rest, rest, p_s, p_r, beside).wait()


def conclude(n, formed, power, bands, beams, decibels, level, sems):
    pieces = sems.shape[0] - 1
    rows = formed.shape[0] // pieces
    copies = []
    for i in range(pieces):
        span = pl.ds(i * rows, rows)
        copies.append(pltpu.make_async_copy(formed.at[span], beams.at[span], sems.at[i]))
        copies[-1].start()
    low, size = bands[0], bands[1]
    high = low + size
    summed = jnp.zeros(level.shape, jnp.float32)
    for u in range(n):
        inside = jnp.logical_and(low <= u, u < high)
        summed = summed + jnp.where(inside, power[u], 0.0)
    mean = summed / (size.astype(jnp.float32) * formed.shape[0])
    level[...] = (10.0 / math.log(10.0)) * jnp.log(mean + epsilon)
    copies.append(pltpu.make_async_copy(level, decibels, sems.at[pieces]))
    copies[-1].start()
    for copy in copies:
        copy.wait()


def local_ring(n, snapshots, delays, element_order, beam_table, band_len):
    local_elems = snapshots.shape[1]
    unit_cols = snapshots.shape[2] // n
    beams = beam_table.shape[0]
    most, chunk = CHUNKS - 1, unit_cols // CHUNKS
    block = (2 * beams, chunk)
    f32, sem = jnp.float32, pltpu.SemaphoreType.DMA
    raw = (2, local_elems)
    vmem, hbm = (pl.BlockSpec(memory_space=m) for m in (pltpu.VMEM, pl.ANY))
    band_shape = (band_len.shape[0], beams)
    formed, power, bands = pl.pallas_call(
        functools.partial(kernel, n),
        out_shape=(
            pltpu.VMEM((unit_cols, 2, beams), f32),
            pltpu.VMEM((n, 1, beams), f32),
            pltpu.VMEM((2,) + band_shape, jnp.int32),
        ),
        in_specs=[hbm] * 5,
        out_specs=(vmem, vmem, vmem),
        scratch_shapes=[
            pltpu.SMEM(band_len.shape, jnp.int32),
            pltpu.VMEM(delays.shape, f32),
            pltpu.VMEM((n, 1, local_elems), jnp.int32),
            pltpu.VMEM((1, beams), jnp.int32),
            pltpu.VMEM((3 * beams, delays.shape[1]), jnp.bfloat16),
            pltpu.VMEM((6, beams, local_elems), f32),
            pltpu.VMEM((2 * beams, 8 * local_elems), jnp.bfloat16),
            pltpu.VMEM((2 * beams, 8 * local_elems), jnp.bfloat16),
            pltpu.VMEM((4, 4) + raw + (most * chunk,), f32),
            pltpu.VMEM((2, 6, 2) + raw + (chunk,), f32),
            pltpu.VMEM((4, 2, 2) + raw + (chunk,), f32),
            pltpu.VMEM((4, most) + block, f32),
            pltpu.VMEM((6, 2) + block, f32),
            pltpu.VMEM((5, most) + block, f32),
            pltpu.VMEM((5, 2) + block, f32),
            pltpu.VMEM((3,) + block, f32),
            pltpu.VMEM(block, f32),
            pltpu.VMEM((1, 2 * beams), f32),
            sem((4,)), sem((4,)), sem((6, 2)),
            sem((4,)), sem((4,)), sem((6, 2)), sem((6, 2)),
            sem((2, 4, most)), sem((2, 4, most)), sem((4, 2, 2)), sem((4, 2, 2)),
            sem((3, most)), sem((5, most)), sem((5, 2)), sem((5, 2)),
            sem((3,)), sem((3,)),
            sem((2, 4)), sem((2, 4)),
            sem, sem,
        ],
        compiler_params=pltpu.CompilerParams(
            collective_id=0, has_side_effects=True, vmem_limit_bytes=54 * 1024 * 1024
        ),
    )(
        band_len, snapshots, delays,
        element_order.reshape(n, 1, local_elems), beam_table.reshape(1, beams),
    )
    parts = [pltpu.with_memory_space_constraint(v, pltpu.VMEM) for v in (formed, power, bands)]
    return pl.pallas_call(
        functools.partial(conclude, n),
        out_shape=(
            jax.ShapeDtypeStruct((unit_cols, 2, beams), f32),
            jax.ShapeDtypeStruct(band_shape, f32),
        ),
        in_specs=[vmem] * 3,
        out_specs=(hbm, hbm),
        scratch_shapes=[pltpu.VMEM(band_shape, f32), sem((9,))],
    )(*parts)


def fits(mesh):
    return mesh.shape["elem"] == SIDE * SIDE * RING


def steering(delays, element_order, beam_table, frequency):
    delay_rows = jnp.take(delays, beam_table, axis=0)
    delay_rows = jnp.take(delay_rows, element_order, axis=1)
    phases = 2.0 * math.pi * frequency * delay_rows
    scaling = float(delays.shape[1]) ** (-0.5)
    cosines = jnp.cos(phases) * scaling
    sines = -jnp.sin(phases) * scaling
    upper_rows = jnp.concatenate([cosines.T, sines.T], axis=1)
    lower_rows = jnp.concatenate([-sines.T, cosines.T], axis=1)
    return jnp.concatenate([upper_rows, lower_rows], axis=0)


def project(arrived, weights):
    columns = arrived.shape[2]
    stacked = arrived.reshape(2 * arrived.shape[1], columns)
    return lax.dot_general(
        stacked,
        weights,
        (((0,), (0,)), ((), ())),
        precision=lax.Precision.HIGHEST,
        preferred_element_type=jnp.float32,
    )


def local(snapshots, delays, element_order, beam_table, band_len):
    unit_count = lax.axis_size("elem")
    position = lax.axis_index("elem")
    frequency, band_size, selector = band_of(band_len, position, unit_count)
    weights = steering(delays, element_order, beam_table, frequency)
    beam_count = beam_table.shape[0]
    local_elems = snapshots.shape[1]
    unit_cols = snapshots.shape[2] // unit_count
    divided = snapshots.reshape(2, local_elems, unit_count, unit_cols)
    pieces = lax.all_to_all(divided, "elem", split_axis=2, concat_axis=1, tiled=True)
    formed = project(pieces.reshape(2, pieces.shape[1], pieces.shape[3]), weights)
    column_count = formed.shape[0]
    squares = jnp.sum(formed * formed, axis=0)
    power_mean = (squares[:beam_count] + squares[beam_count:]) / (
        band_size.astype(jnp.float32) * column_count
    )
    partial_value = selector[:, None] * power_mean[None, :]
    summed = lax.psum(partial_value, "elem")
    decibels = 10.0 * jnp.log10(summed + epsilon)
    return (formed.reshape(column_count, 2, beam_count), decibels)


def solution(mesh):
    n = mesh.shape["elem"]
    body = functools.partial(local_ring, n) if fits(mesh) else local
    return jax.shard_map(
        body,
        mesh=mesh,
        in_specs=(P(None, ("groups", "elem"), None), P(), P("groups"), P("groups"), P()),
        out_specs=(P("elem", None, "groups"), P(None, "groups")),
        check_vma=False,
    )
```
